256 devices in a mesh: dp: 8 (over y, x_lo), seq: 32 (over z, x_hi, core).
Axes of the slice: x: 4 (x_hi: 2, x_lo: 2; x = x_hi * 2 + x_lo), y: 4, z: 8, core: 2. Of those that a mesh axis runs over, the one named last changes fastest.
Arguments:
- tokens: bfloat16 [8, 16384, 2560], P('dp', 'seq'), may hold values from -6 to 6
- w_x: bfloat16 [2560, 3072], P('seq'), may hold values from -0.125 to 0.125
- w_bc: bfloat16 [2560, 256], P('seq'), may hold values from -0.125 to 0.125
- w_dt: bfloat16 [2560, 48], P('seq'), may hold values from -0.125 to 0.125
- dt_bias: float32 [48], replicated, may hold values from -1 to 0.5
- decay_rate: float32 [48], replicated, may hold values from 2.4414063e-05 to 0.12
- gain: float32 [3072], replicated, may hold values from 0.5 to 1.5
- cotangent: bfloat16 [8, 16384, 3072], P('dp', 'seq'), may hold values from -0.005859375 to 0.005859375
- counts: int32 [32], replicated, may hold values from 1 to 2, 48 in all
Outputs:
- ssm_output: bfloat16 [8, 16384, 3072], P('dp', 'seq')
- grad_c: float32 [2560, 128], P('seq')
The draws below stay inside these ranges and needn't reach their ends.
Inputs may be any that keep to these rules, and one draw needn't show every extreme that they name: counts add up to 48 and one of them equals 2.
All inputs are finite; a program needn't handle non-finite values.
Results may differ from the reference program's by a relative error of at most 0.02.
Values may be sent and summed in bfloat16 or wider, within the bound.
A program may use at most 128 MiB of HBM per device.

```python
import math
import jax
import jax.numpy as jnp
import numpy as np
from jax import lax

D = 2560
H = 48
P_SIZE = 64
N = 128
L = 256
CAP = 2
GROUPS = 32
BATCH = 8
TOTAL = 48
ROWS = 16384


def draw_decay_rate(key, part):
    key_kind = jax.random.fold_in(key, 11)
    key_slow = jax.random.fold_in(key, 12)
    key_fast = jax.random.fold_in(key, 13)
    key_middle = jax.random.fold_in(key, 14)
    slow_share = 0.4
    middle_share = 0.3
    picker = jax.random.uniform(key_kind, (H,))
    slow_rate = jnp.exp(jax.random.uniform(key_slow, (H,), minval=math.log(0.3), maxval=math.log(2.0))) / (TOTAL * L)
    middle_rate = jnp.exp(jax.random.uniform(key_middle, (H,), minval=math.log(0.0015), maxval=math.log(0.006)))
    fast_rate = jnp.exp(jax.random.uniform(key_fast, (H,), minval=math.log(0.04), maxval=math.log(0.12)))
    chosen = jnp.where(picker < slow_share, slow_rate, jnp.where(picker < slow_share + middle_share, middle_rate, fast_rate))
    return chosen.astype(jnp.float32)


def block_levels(key, dims, pieces, smallest, top_value):
    level = 1.0
    for axis_at, blocks in pieces:
        draws = jax.random.uniform(jax.random.fold_in(jax.random.fold_in(key, 6), axis_at), (blocks,), jnp.float32, smallest / len(pieces), top_value / len(pieces))
        level = level * jnp.repeat(jnp.exp(draws), dims[axis_at] // blocks).reshape((-1,) + (1,) * (len(dims) - 1 - axis_at))
    return level


def profile(amount, total, limit, skew):
    portions = [(1 << 20) // math.isqrt(standing ** skew) + 1 for standing in range(2, amount + 1)]
    spare, given = total - limit - (amount - 1), [1] * (amount - 1)
    while spare > 0:
        candidates = [i for i in range(amount - 1) if given[i] < limit]
        whole, left = sum([portions[i] for i in candidates]), spare
        for i in candidates:
            addition = min(limit - given[i], max(1, left * portions[i] // whole), spare)
            given[i] = given[i] + addition
            spare = spare - addition
    return np.array([limit] + given)


def ragged(key, number_of, total, reach, slope):
    if number_of == 2:
        one = jax.random.randint(key, (), max(1, total - reach), min(reach, total - 1) + 1)
        return jnp.stack([one, total - one])
    sizes = jnp.asarray(profile(number_of, total, reach, slope), jnp.int32)
    twos = (number_of - 1) // 2
    source_of, taker = sizes[1:1 + 2 * twos:2], sizes[2:2 + 2 * twos:2]
    slack = jnp.minimum(source_of - 1, reach - taker)
    moved = jax.random.randint(jax.random.fold_in(key, 1), (twos,), 0, 1 << 20) % (slack + 1)
    sizes = sizes.at[1:1 + 2 * twos:2].set(source_of - moved).at[2:2 + 2 * twos:2].set(taker + moved)
    return sizes[jax.random.permutation(jax.random.fold_in(key, 2), number_of)]


def scatter_about(stream_key, shape, scale, reach, split=(), dtype=jnp.bfloat16):
    level = block_levels(stream_key, shape, split, -0.22, 0.18) if split else 1.0
    drawn = jax.random.normal(stream_key, shape, jnp.float32) * scale * level
    return jnp.minimum(jnp.maximum(drawn, -reach), reach).astype(dtype)


def setup_inputs(seed: int = 0) -> dict:
    splits = jax.random.split(jax.random.key(seed), 10)
    return {
        "tokens": scatter_about(splits[0], (BATCH, ROWS, D), 1.0, 6.0, ((0, 8), (1, 32))),
        "w_x": scatter_about(splits[1], (D, H * P_SIZE), D ** -0.5, 0.125, ((0, 32),)),
        "w_bc": scatter_about(splits[2], (D, 2 * N), D ** -0.5, 0.125, ((0, 32),)),
        "w_dt": scatter_about(splits[3], (D, H), D ** -0.5, 0.125, ((0, 32),)),
        "dt_bias": jnp.clip(jax.random.uniform(splits[4], (H,), jnp.float32, -1.0, 0.5), -1.0, 0.5),
        "decay_rate": draw_decay_rate(jax.random.fold_in(splits[9], 71), 0),
        "gain": jnp.clip(1.0 + 0.1 * jax.random.normal(splits[6], (H * P_SIZE,), jnp.float32), 0.5, 1.5),
        "cotangent": scatter_about(splits[7], (BATCH, ROWS, H * P_SIZE), 0.001, 0.005859375, ((0, 8), (1, 32))),
        "counts": ragged(splits[8], GROUPS, TOTAL, CAP, 1).astype(jnp.int32),
    }


norm_floor = 1.0

def decay_weights(cumulative, dt_rows):
    length = cumulative.shape[0]
    causal = jnp.arange(length)[:, None] >= jnp.arange(length)[None, :]
    gap_log = cumulative.T[:, :, None] - cumulative.T[:, None, :]
    gap_log = jnp.where(causal[None, :, :], gap_log, -jnp.inf)
    return jnp.exp(gap_log) * dt_rows.T[:, None, :]

def stretch_state(inner, b_proj, dt_rows, a_neg):
    length = inner.shape[0]
    head_count = a_neg.shape[0]
    cumulative = jnp.cumsum(dt_rows * a_neg[None, :], axis=0)
    to_end = jnp.exp(cumulative[-1][None, :] - cumulative) * dt_rows
    scaled = (inner.astype(jnp.float32).reshape(length, head_count, -1) * to_end[:, :, None]).reshape(length, -1).astype(jnp.bfloat16)
    state_add = jnp.dot(scaled.T, b_proj, preferred_element_type=jnp.float32)
    return (jnp.exp(cumulative[-1]), state_add)

def stretch_outputs(inner, b_proj, c_proj, dt_rows, a_neg, state_in, gain, cot_rows, slot_used):
    length = inner.shape[0]
    head_count = a_neg.shape[0]
    head_size = inner.shape[1] // head_count
    cumulative = jnp.cumsum(dt_rows * a_neg[None, :], axis=0)
    weights = decay_weights(cumulative, dt_rows)
    gram_mat = jnp.dot(c_proj, b_proj.T, preferred_element_type=jnp.float32)
    mixing = (gram_mat[None, :, :] * weights).astype(jnp.bfloat16)
    inner_heads = inner.reshape(length, head_count, head_size)
    y_intra = jnp.einsum('hts,shp->thp', mixing.astype(jnp.float32), inner_heads.astype(jnp.float32))
    state_low = state_in.astype(jnp.bfloat16)
    growth = jnp.exp(cumulative)[:, :, None]
    y_inter = jnp.dot(c_proj, state_low.T, preferred_element_type=jnp.float32).reshape(length, head_count, head_size) * growth
    full = y_intra + y_inter
    radius = jnp.sqrt(lax.optimization_barrier(jnp.mean(full * full, axis=2, keepdims=True)) + norm_floor)
    gain_heads = gain.reshape(head_count, head_size)
    output = (full / radius * gain_heads * slot_used).reshape(length, -1).astype(jnp.bfloat16)
    grad_out = cot_rows.astype(jnp.float32).reshape(length, head_count, head_size) * gain_heads
    grad_full = (grad_out / radius - full * lax.optimization_barrier(jnp.sum(grad_out * full, axis=2, keepdims=True)) / (head_size * radius ** 3)) * slot_used
    grad_low = grad_full.astype(jnp.bfloat16)
    intersect = jnp.einsum('thp,shp->hts', grad_low.astype(jnp.float32), inner_heads.astype(jnp.float32))
    combined = lax.optimization_barrier(jnp.sum(intersect * weights, axis=0)).astype(jnp.bfloat16)
    grad_intra = jnp.dot(combined, b_proj, preferred_element_type=jnp.float32)
    scaled_grad = (grad_full * growth).reshape(length, -1).astype(jnp.bfloat16)
    grad_inter = jnp.dot(scaled_grad, state_low, preferred_element_type=jnp.float32)
    return (output, (grad_intra + grad_inter).astype(jnp.bfloat16))

def reference(tokens, w_x, w_bc, w_dt, dt_bias, decay_rate, gain, cotangent, counts):
    batch = tokens.shape[0]
    slot_total = tokens.shape[1] // L
    state_size = w_bc.shape[1] // 2
    head_count = decay_rate.shape[0]
    a_neg = -decay_rate
    token_blocks = tokens.reshape(batch, slot_total, L, -1).transpose(1, 0, 2, 3)
    cotangent_blocks = cotangent.reshape(batch, slot_total, L, -1).transpose(1, 0, 2, 3)
    slot_ids = jnp.arange(slot_total).astype(jnp.int32)
    filled = counts[slot_ids // CAP]
    slot_used = (slot_ids % CAP < filled).astype(jnp.float32)

    def advance(running, stretch_data):
        states, gradient = running
        token_rows, cot_rows, used = stretch_data
        inner = jnp.dot(token_rows, w_x, preferred_element_type=jnp.float32).astype(jnp.bfloat16)
        bc_raw = jnp.dot(token_rows, w_bc, preferred_element_type=jnp.float32)
        b_proj = bc_raw[:, :, :state_size].astype(jnp.bfloat16)
        c_proj = bc_raw[:, :, state_size:].astype(jnp.bfloat16)
        dt_rows = jax.nn.softplus(jnp.dot(token_rows, w_dt, preferred_element_type=jnp.float32) + dt_bias) * used
        decays, state_add = jax.vmap(stretch_state, in_axes=(0, 0, 0, None))(inner, b_proj, dt_rows, a_neg)
        output, grad_rows = jax.vmap(stretch_outputs, in_axes=(0, 0, 0, 0, None, 0, None, 0, None))(inner, b_proj, c_proj, dt_rows, a_neg, states, gain, cot_rows, used)
        gradient = gradient + jnp.einsum('btd,btn->dn', token_rows.astype(jnp.float32), grad_rows.astype(jnp.float32))
        states = (states.reshape(batch, head_count, -1) * decays[:, :, None]).reshape(states.shape) + state_add
        return ((states, gradient), output)
    starting = (jnp.zeros((batch, w_x.shape[1], state_size), jnp.float32), jnp.zeros((tokens.shape[2], state_size), jnp.float32))
    (unused, gradient), outputs = lax.scan(advance, starting, (token_blocks, cotangent_blocks, slot_used))
    ssm_output = outputs.transpose(1, 0, 2, 3).reshape(batch, tokens.shape[1], -1)
    return (ssm_output, gradient)
```

```python
import functools

import jax
import jax.numpy as jnp
from jax import lax
from jax.experimental import pallas as pl
from jax.experimental.pallas import tpu as pltpu
from jax.sharding import Mesh
from jax.sharding import PartitionSpec as P

L = 256
CHUNK = 128
WIDE = 256
SEQ = ("seq_0", "seq_1", "seq_2")
LOG2E = 1.4426950408889634
F32 = jnp.float32
BF16 = jnp.bfloat16


def dot(a, b):
    return jnp.dot(a, b, preferred_element_type=F32)


def dot_lanes(a, b):
    return lax.dot_general(a, b, (((1,), (1,)), ((), ())), preferred_element_type=F32)


def iota(shape, dim):
    return lax.broadcasted_iota(jnp.int32, shape, dim)


def split3(x):
    hi = x.astype(BF16).astype(F32)
    mid = (x - hi).astype(BF16).astype(F32)
    return hi, mid, x - hi - mid


def packed3(x):
    hi, mid, lo = split3(x)
    low_lanes = iota(x.shape, 1) < 64
    first = jnp.where(low_lanes, hi, pltpu.roll(mid, 64, 1))
    second = jnp.where(low_lanes, lo, 0.0)
    return jnp.concatenate([first.astype(BF16), second.astype(BF16)], axis=1)


def head_select(depth, first_head, lanes_per_head):
    k = iota((depth, WIDE), 0)
    l = iota((depth, WIDE), 1)
    hit = ((k & 63) == first_head + l // lanes_per_head) & (k < 192)
    return jnp.where(hit, 1.0, 0.0).astype(BF16)


def state_kernel(dt_ref, bias_ref, rate_ref, used_ref, b_ref, inner_ref,
                 prior_ref, total_ref, pre_ref, cum_ref, row_ref, to_end, ends, b_turned):
    step = pl.program_id(0)
    rows = dt_ref.shape[0]
    chunks = rows // CHUNK

    @pl.when(step == 0)
    def _():
        v = dt_ref[...] + bias_ref[...]
        dt = jnp.maximum(v, 0.0) + jnp.log1p(jnp.exp(-jnp.abs(v)))
        slot = iota(dt.shape, 0) // L
        dt = dt * jnp.where(slot == 0, used_ref[0, 0], used_ref[0, 1])
        drop = dt * (rate_ref[...] * (-LOG2E))
        tri = jnp.where(iota((CHUNK, CHUNK), 0) >= iota((CHUNK, CHUNK), 1), 1.0, 0.0).astype(BF16)
        lasts = []
        for c in range(chunks):
            at = slice(c * CHUNK, (c + 1) * CHUNK)
            hi, mid, lo = split3(drop[at])
            cum = dot(tri, hi.astype(BF16)) + dot(tri, mid.astype(BF16)) + dot(tri, lo.astype(BF16))
            own = cum - jnp.log2(dt[at])
            last = cum[CHUNK - 1:CHUNK]
            lasts.append(last)
            cum_ref[at, :] = packed3(cum)
            reach = jnp.exp2(last - own)
            reach_hi = reach.astype(BF16).astype(F32)
            reach_lo = pltpu.roll(reach - reach_hi, 64, 1)
            to_end[at, :] = jnp.where(iota(reach.shape, 1) < 64, reach_hi, reach_lo).astype(BF16)
            turned = own.T
            for g in range(row_ref.shape[0]):
                row_ref[g, :, at] = turned[4 * g:4 * g + 4]
            b_turned[c] = b_ref[at, :].astype(F32).T.astype(BF16)
        lasts = jnp.concatenate(lasts + [jnp.zeros((16 - chunks, CHUNK), F32)], axis=0)
        ends[...] = packed3(lasts)

    first_head = step * (WIDE // 64)
    reach = dot(to_end[...], head_select(CHUNK, first_head, 64))
    scaled = (inner_ref[...].astype(F32) * reach).astype(BF16)
    decay = jnp.exp2(dot(ends[...], head_select(2 * CHUNK, first_head, 64)))
    state, before = None, jnp.ones((1, WIDE), F32)
    for c in range(chunks):
        add = dot(b_turned[c], scaled[c * CHUNK:(c + 1) * CHUNK])
        here = decay[c:c + 1]
        if c == 0:
            state = add
        else:
            prior_ref[c - 1] = state
            state = state * here + add
        pre_ref[c:c + 1, :] = before
        before = before * here
    pre_ref[chunks:chunks + 1, :] = before
    total_ref[...] = state.astype(total_ref.dtype)


def output_kernel(cum_ref, row_ref, c_ref, b_ref, tokens_ref, inner_ref, cot_ref, gain_ref,
                  prior_ref, pre_ref, enter_ref, out_ref, grad_ref, gram, hide, sum_heads, combined, through):
    step = pl.program_id(0)
    rows = c_ref.shape[0]
    chunks = rows // CHUNK

    @pl.when(step == 0)
    def _():
        for c in range(chunks):
            at = slice(c * CHUNK, (c + 1) * CHUNK)
            gram[at, :] = dot_lanes(c_ref[at, :], b_ref[at, :])
        hide[...] = jnp.where(iota(hide.shape, 0) >= iota(hide.shape, 1), 0.0, -1e30)
        same = iota(sum_heads.shape, 0) // 64 == iota(sum_heads.shape, 1) // 64
        sum_heads[...] = jnp.where(same, 1.0, 0.0).astype(BF16)
        combined[...] = jnp.zeros_like(combined)
        through[...] = jnp.zeros_like(through)

    first_head = step * 4
    low_half = iota((CHUNK, CHUNK), 1) < 64
    spread = [dot(cum_ref[...], head_select(2 * CHUNK, first_head + 2 * p, CHUNK)) for p in range(2)]
    for c in range(chunks):
        at = slice(c * CHUNK, (c + 1) * CHUNK)
        entering = enter_ref[...] * pre_ref[c:c + 1, :]
        if c > 0:
            entering = entering + prior_ref[c - 1]
        state_low = entering.astype(BF16)
        from_state = dot(c_ref[at, :], state_low)
        gain_row = gain_ref[c * CHUNK // L:c * CHUNK // L + 1, :]
        scaled = []
        for p in range(2):
            lanes = slice(p * CHUNK, (p + 1) * CHUNK)
            cum0, cum1 = spread[p][at, :CHUNK], spread[p][at, CHUNK:]
            w0 = jnp.exp2(cum0 - row_ref[0, 2 * p:2 * p + 1, at] + hide[...])
            w1 = jnp.exp2(cum1 - row_ref[0, 2 * p + 1:2 * p + 2, at] + hide[...])
            dots = gram[at, :]
            mixing = jnp.concatenate([(dots * w0).astype(BF16), (dots * w1).astype(BF16)], axis=1)
            x = inner_ref[at, lanes]
            zero = jnp.zeros_like(x)
            heads = jnp.concatenate([jnp.where(low_half, x, zero), jnp.where(low_half, zero, x)], axis=0)
            growth = jnp.exp2(jnp.where(low_half, cum0, cum1))
            full = dot(mixing, heads) + from_state[:, lanes] * growth
            gain = gain_row[:, lanes]
            grad_out = cot_ref[at, lanes].astype(F32) * gain
            parts = jnp.concatenate([(full * full).astype(BF16), (grad_out * full).astype(BF16)], axis=1)
            sums = dot(parts, sum_heads[...])
            inverse = lax.rsqrt(sums[:, :CHUNK] * (1.0 / 64) + 1.0)
            normed = full * inverse
            out_ref[at, lanes] = (normed * gain).astype(BF16)
            grad = inverse * (grad_out - normed * (sums[:, CHUNK:] * inverse * (1.0 / 64)))
            inter = dot_lanes(grad.astype(BF16), heads)
            combined[at, :] += inter[:, :CHUNK] * w0 + inter[:, CHUNK:] * w1
            scaled.append((grad * growth).astype(BF16))
        through[at, :] += dot_lanes(jnp.concatenate(scaled, axis=1), state_low)

    @pl.when(step == pl.num_programs(0) - 1)
    def _():
        turned = []
        for c in range(chunks):
            at = slice(c * CHUNK, (c + 1) * CHUNK)
            grad_rows = dot(combined[at, :].astype(BF16), b_ref[at, :]) + through[at, :]
            turned.append(grad_rows.astype(BF16).astype(F32).T.astype(BF16))
        turned = jnp.concatenate(turned, axis=1)
        for k in range(grad_ref.shape[0] // CHUNK):
            at = slice(k * CHUNK, (k + 1) * CHUNK)
            grad_ref[at, :] = dot(turned, tokens_ref[:, at]).T.astype(grad_ref.dtype)


def whole(shape):
    return pl.BlockSpec(shape, lambda j: (0,) * len(shape))


def local_states(dt_raw, dt_bias, decay_rate, used, b_proj, inner):
    rows, width = inner.shape
    state_size = b_proj.shape[1]
    steps = width // WIDE
    chunks = rows // CHUNK
    pad = 128 - dt_bias.shape[0]
    bias = jnp.pad(dt_bias, (0, pad))[None]
    rate = jnp.pad(decay_rate, (0, pad))[None]
    columns = lambda r: pl.BlockSpec((r, WIDE), lambda j: (0, j))
    return pl.pallas_call(
        state_kernel,
        grid=(steps,),
        out_shape=(
            jax.ShapeDtypeStruct((chunks - 1, state_size, width), F32),
            jax.ShapeDtypeStruct((state_size, width), BF16),
            jax.ShapeDtypeStruct((8, width), F32),
            jax.ShapeDtypeStruct((rows, 2 * CHUNK), BF16),
            jax.ShapeDtypeStruct((steps, 4, rows), F32),
        ),
        in_specs=[
            whole((rows, 128)), whole((1, 128)), whole((1, 128)),
            pl.BlockSpec(memory_space=pltpu.SMEM),
            whole((rows, state_size)), columns(rows),
        ],
        out_specs=(
            pl.BlockSpec((chunks - 1, state_size, WIDE), lambda j: (0, 0, j)),
            columns(state_size), columns(8), whole((rows, 2 * CHUNK)), whole((steps, 4, rows)),
        ),
        scratch_shapes=[
            pltpu.VMEM((rows, CHUNK), BF16),
            pltpu.VMEM((16, 2 * CHUNK), BF16),
            pltpu.VMEM((chunks, state_size, CHUNK), BF16),
        ],
        name="states",
    )(dt_raw, bias, rate, used, b_proj, inner)


def local_outputs(cum, row, c_proj, b_proj, tokens, inner, cot, gain, prior, pre, entering):
    rows, width = inner.shape
    depth = tokens.shape[1]
    state_size = b_proj.shape[1]
    steps = width // WIDE
    chunks = rows // CHUNK
    columns = lambda r: pl.BlockSpec((r, WIDE), lambda j: (0, j))
    return pl.pallas_call(
        output_kernel,
        grid=(steps,),
        out_shape=(
            jax.ShapeDtypeStruct((rows, width), BF16),
            jax.ShapeDtypeStruct((depth, state_size), BF16),
        ),
        in_specs=[
            whole((rows, 2 * CHUNK)), pl.BlockSpec((1, 4, rows), lambda j: (j, 0, 0)),
            whole((rows, state_size)), whole((rows, state_size)), whole((rows, depth)),
            columns(rows), columns(rows), columns(gain.shape[0]),
            pl.BlockSpec((chunks - 1, state_size, WIDE), lambda j: (0, 0, j)), columns(8), columns(state_size),
        ],
        out_specs=(columns(rows), whole((depth, state_size))),
        scratch_shapes=[
            pltpu.VMEM((rows, CHUNK), F32),
            pltpu.VMEM((CHUNK, CHUNK), F32),
            pltpu.VMEM((WIDE, WIDE), BF16),
            pltpu.VMEM((rows, CHUNK), F32),
            pltpu.VMEM((rows, CHUNK), F32),
        ],
        name="outputs",
    )(cum, row, c_proj, b_proj, tokens, inner, cot, gain, prior, pre, entering)


def entering_state(decay, state, axes):
    before = jnp.zeros(state.shape, F32)
    sub_decay, sub_state = decay, state.astype(F32)
    for axis in reversed(axes):
        peers, place = lax.axis_size(axis), lax.axis_index(axis)
        decays = lax.all_gather(sub_decay, axis)
        states = lax.all_gather(sub_state.astype(BF16), axis)
        inside_d, inside_s = jnp.ones_like(decay), jnp.zeros(state.shape, F32)
        sub_decay, sub_state = jnp.ones_like(decay), jnp.zeros(state.shape, F32)
        own_d, own_s = sub_decay, sub_state
        for k in range(peers):
            own_d = jnp.where(k == place, sub_decay, own_d)
            own_s = jnp.where(k == place, sub_state, own_s)
            sub_state = sub_state * decays[k] + states[k].astype(F32)
            sub_decay = sub_decay * decays[k]
        inside_d, inside_s = own_d, own_s
        if axis == axes[-1]:
            total_d, before = inside_d, inside_s
        else:
            before = inside_s * total_d + before
            total_d = inside_d * total_d
    return before


def cut_along(shard, dim, peers):
    shape = shard.shape
    blocks = shard.reshape(*shape[:dim], peers, shape[dim] // peers, *shape[dim + 1:])
    return jnp.moveaxis(blocks, dim, 0)


def sum_at_owner(shard, axis, dim):
    blocks = cut_along(shard, dim, lax.axis_size(axis))
    arrived = lax.all_to_all(blocks, axis, split_axis=0, concat_axis=0, tiled=True)
    return arrived.astype(F32).sum(axis=0)


def copy_for_each(shard, axis):
    peers = lax.axis_size(axis)
    return lax.all_to_all(jnp.broadcast_to(shard[None], (peers, *shard.shape)), axis, 0, 0, tiled=True)


def body(tokens, w_x, w_bc, w_dt, dt_bias, decay_rate, gain, cotangent, counts):
    seq_tokens = tokens[0]
    cot_rows = cotangent[0]
    slot_count = seq_tokens.shape[0] // L
    state_size = w_bc.shape[1] // 2
    group_index = lax.axis_index(SEQ)
    filled = jnp.sum(jnp.where(jnp.arange(counts.shape[0]) == group_index, counts, 0))
    slot_used = (jnp.arange(slot_count) < filled).astype(F32)
    pad = jnp.zeros((w_dt.shape[0], 128 - w_dt.shape[1]), BF16)
    pieces = lax.all_gather(jnp.concatenate([w_x, w_bc, w_dt, pad], axis=1), SEQ, axis=0, tiled=True)
    width = w_x.shape[1]
    inner = dot(seq_tokens, pieces[:, :width]).astype(BF16)
    bc_raw = dot(seq_tokens, pieces[:, width:width + 2 * state_size]).astype(BF16)
    dt_raw = dot(seq_tokens, pieces[:, width + 2 * state_size:])
    b_proj, c_proj = bc_raw[:, :state_size], bc_raw[:, state_size:]
    prior, total, pre, cum, row = local_states(dt_raw, dt_bias, decay_rate, slot_used[None], b_proj, inner)
    chunks = seq_tokens.shape[0] // CHUNK
    entering = entering_state(pre[chunks:chunks + 1], total, SEQ)
    gains = gain[None] * slot_used[:, None]
    outputs, grad = local_outputs(cum, row, c_proj, b_proj, seq_tokens, inner, cot_rows, gains, prior, pre, entering)
    partial_rows = sum_at_owner(grad, SEQ, 0)
    gradient = copy_for_each(partial_rows.astype(BF16), "dp").astype(F32).sum(axis=0)
    return (outputs[None], gradient)


def solution(mesh):
    finer = Mesh(mesh.devices.reshape(mesh.shape["dp"], 8, 2, 2), ("dp", "seq_0", "seq_1", "seq_2"))
    return jax.shard_map(
        body,
        mesh=finer,
        in_specs=(
            P("dp", SEQ, None), P(SEQ, None), P(SEQ, None), P(SEQ, None),
            P(), P(), P(), P("dp", SEQ, None), P(),
        ),
        out_specs=(P("dp", SEQ, None), P(SEQ, None)),
        check_vma=False,
    )
```

```python
import functools

import jax
import jax.numpy as jnp
from jax import lax
from jax.experimental import pallas as pl
from jax.experimental.pallas import tpu as pltpu
from jax.sharding import Mesh
from jax.sharding import PartitionSpec as P

L = 256
CHUNK = 128
WIDE = 256
LOG2E = 1.4426950408889634
F32 = jnp.float32
BF16 = jnp.bfloat16


def dot(a, b):
    return jnp.dot(a, b, preferred_element_type=F32)


def dot_lanes(a, b):
    return lax.dot_general(a, b, (((1,), (1,)), ((), ())), preferred_element_type=F32)


def iota(shape, dim):
    return lax.broadcasted_iota(jnp.int32, shape, dim)


def split3(x):
    hi = x.astype(BF16).astype(F32)
    mid = (x - hi).astype(BF16).astype(F32)
    return hi, mid, x - hi - mid


def packed3(x):
    hi, mid, lo = split3(x)
    low_lanes = iota(x.shape, 1) < 64
    first = jnp.where(low_lanes, hi, pltpu.roll(mid, 64, 1))
    second = jnp.where(low_lanes, lo, 0.0)
    return jnp.concatenate([first.astype(BF16), second.astype(BF16)], axis=1)


def head_select(depth, first_head, lanes_per_head):
    k = iota((depth, WIDE), 0)
    l = iota((depth, WIDE), 1)
    hit = ((k & 63) == first_head + l // lanes_per_head) & (k < 192)
    return jnp.where(hit, 1.0, 0.0).astype(BF16)


def state_kernel(dt_ref, bias_ref, rate_ref, used_ref, b_ref, inner_ref,
                 prior_ref, total_ref, decay_ref, pre_ref, cum_ref, row_ref, to_end, ends, b_turned):
    step = pl.program_id(0)
    rows = dt_ref.shape[0]
    chunks = rows // CHUNK

    @pl.when(step == 0)
    def _():
        v = dt_ref[...] + bias_ref[...]
        dt = jnp.maximum(v, 0.0) + jnp.log1p(jnp.exp(-jnp.abs(v)))
        slot = iota(dt.shape, 0) // L
        dt = dt * jnp.where(slot == 0, used_ref[0, 0], used_ref[0, 1])
        drop = dt * (rate_ref[...] * (-LOG2E))
        tri = jnp.where(iota((CHUNK, CHUNK), 0) >= iota((CHUNK, CHUNK), 1), 1.0, 0.0).astype(BF16)
        lasts = []
        for c in range(chunks):
            at = slice(c * CHUNK, (c + 1) * CHUNK)
            hi, mid, lo = split3(drop[at])
            cum = dot(tri, hi.astype(BF16)) + dot(tri, mid.astype(BF16)) + dot(tri, lo.astype(BF16))
            own = cum - jnp.log2(dt[at])
            last = cum[CHUNK - 1:CHUNK]
            lasts.append(last)
            cum_ref[at, :] = packed3(cum)
            reach = jnp.exp2(last - own)
            reach_hi = reach.astype(BF16).astype(F32)
            reach_lo = pltpu.roll(reach - reach_hi, 64, 1)
            to_end[at, :] = jnp.where(iota(reach.shape, 1) < 64, reach_hi, reach_lo).astype(BF16)
            turned = own.T
            for g in range(row_ref.shape[0]):
                row_ref[g, :, at] = turned[4 * g:4 * g + 4]
            b_turned[c] = b_ref[at, :].astype(F32).T.astype(BF16)
        lasts = jnp.concatenate(lasts + [jnp.zeros((16 - chunks, CHUNK), F32)], axis=0)
        ends[...] = packed3(lasts)

    first_head = step * (WIDE // 64)
    reach = dot(to_end[...], head_select(CHUNK, first_head, 64))
    scaled = (inner_ref[...].astype(F32) * reach).astype(BF16)
    decay = jnp.exp2(dot(ends[...], head_select(2 * CHUNK, first_head, 64)))
    state, before = None, jnp.ones((1, WIDE), F32)
    for c in range(chunks):
        add = dot(b_turned[c], scaled[c * CHUNK:(c + 1) * CHUNK])
        here = decay[c:c + 1]
        if c == 0:
            state = add
        else:
            prior_ref[c - 1] = state
            state = state * here + add
        pre_ref[c:c + 1, :] = before
        before = before * here
    for p in range(WIDE // CHUNK):
        lanes = slice(p * CHUNK, (p + 1) * CHUNK)
        total_ref[p] = state[:, lanes].astype(total_ref.dtype)
        decay_ref[pl.ds(step * (WIDE // CHUNK) + p, 1), :] = before[:, lanes]


def output_kernel(cum_ref, row_ref, c_ref, b_ref, tokens_ref, inner_ref, cot_ref, gain_ref,
                  prior_ref, pre_ref, enter_ref, out_ref, grad_ref, gram, hide, sum_heads, combined, through):
    step = pl.program_id(0)
    rows = c_ref.shape[0]
    chunks = rows // CHUNK

    @pl.when(step == 0)
    def _():
        for c in range(chunks):
            at = slice(c * CHUNK, (c + 1) * CHUNK)
            gram[at, :] = dot_lanes(c_ref[at, :], b_ref[at, :])
        hide[...] = jnp.where(iota(hide.shape, 0) >= iota(hide.shape, 1), 0.0, -1e30)
        same = iota(sum_heads.shape, 0) // 64 == iota(sum_heads.shape, 1) // 64
        sum_heads[...] = jnp.where(same, 1.0, 0.0).astype(BF16)
        combined[...] = jnp.zeros_like(combined)
        through[...] = jnp.zeros_like(through)

    first_head = step * 4
    low_half = iota((CHUNK, CHUNK), 1) < 64
    spread = [dot(cum_ref[...], head_select(2 * CHUNK, first_head + 2 * p, CHUNK)) for p in range(2)]
    entry = jnp.concatenate([enter_ref[p].astype(F32) for p in range(2)], axis=1)
    for c in range(chunks):
        at = slice(c * CHUNK, (c + 1) * CHUNK)
        entering = entry * pre_ref[c:c + 1, :]
        if c > 0:
            entering = entering + prior_ref[c - 1]
        state_low = entering.astype(BF16)
        from_state = dot(c_ref[at, :], state_low)
        gain_row = gain_ref[c * CHUNK // L:c * CHUNK // L + 1, :]
        scaled = []
        for p in range(2):
            lanes = slice(p * CHUNK, (p + 1) * CHUNK)
            cum0, cum1 = spread[p][at, :CHUNK], spread[p][at, CHUNK:]
            w0 = jnp.exp2(cum0 - row_ref[0, 2 * p:2 * p + 1, at] + hide[...])
            w1 = jnp.exp2(cum1 - row_ref[0, 2 * p + 1:2 * p + 2, at] + hide[...])
            dots = gram[at, :]
            mixing = jnp.concatenate([(dots * w0).astype(BF16), (dots * w1).astype(BF16)], axis=1)
            x = inner_ref[at, lanes]
            zero = jnp.zeros_like(x)
            heads = jnp.concatenate([jnp.where(low_half, x, zero), jnp.where(low_half, zero, x)], axis=0)
            growth = jnp.exp2(jnp.where(low_half, cum0, cum1))
            full = dot(mixing, heads) + from_state[:, lanes] * growth
            gain = gain_row[:, lanes]
            grad_out = cot_ref[at, lanes].astype(F32) * gain
            parts = jnp.concatenate([(full * full).astype(BF16), (grad_out * full).astype(BF16)], axis=1)
            sums = dot(parts, sum_heads[...])
            inverse = lax.rsqrt(sums[:, :CHUNK] * (1.0 / 64) + 1.0)
            normed = full * inverse
            out_ref[at, lanes] = (normed * gain).astype(BF16)
            grad = inverse * (grad_out - normed * (sums[:, CHUNK:] * inverse * (1.0 / 64)))
            inter = dot_lanes(grad.astype(BF16), heads)
            combined[at, :] += inter[:, :CHUNK] * w0 + inter[:, CHUNK:] * w1
            scaled.append((grad * growth).astype(BF16))
        through[at, :] += dot_lanes(jnp.concatenate(scaled, axis=1), state_low)

    @pl.when(step == pl.num_programs(0) - 1)
    def _():
        turned = []
        for c in range(chunks):
            at = slice(c * CHUNK, (c + 1) * CHUNK)
            grad_rows = dot(combined[at, :].astype(BF16), b_ref[at, :]) + through[at, :]
            turned.append(grad_rows.astype(BF16).astype(F32).T.astype(BF16))
        turned = jnp.concatenate(turned, axis=1)
        for k in range(grad_ref.shape[0] // CHUNK):
            at = slice(k * CHUNK, (k + 1) * CHUNK)
            grad_ref[at, :] = dot(turned, tokens_ref[:, at]).T.astype(grad_ref.dtype)


MESH = pl.DeviceIdType.MESH
ZS = 8
CLASSES = {"A": 0, "B": 1, "X": 2, "D": 3}


def place_of():
    dp, seq = lax.axis_index("dp"), lax.axis_index("seq")
    return dict(y=dp // 2, x_lo=lax.rem(dp, 2), z=seq // 4, x_hi=lax.rem(seq // 2, 2), core=lax.rem(seq, 2), seq=seq, dp=dp)


def device_at(place, **new):
    p = {**place, **new}
    return (p["y"] * 2 + p["x_lo"], p["z"] * 4 + p["x_hi"] * 2 + p["core"])


def neighbours(place):
    z, y = place["z"], place["y"]
    flip = 1 - place["x_lo"]
    return dict(
        zp=device_at(place, z=lax.rem(z + 1, ZS)), zm=device_at(place, z=lax.rem(z + ZS - 1, ZS)),
        yp=device_at(place, y=lax.rem(y + 1, 4)), ym=device_at(place, y=lax.rem(y + 3, 4)),
        xu=device_at(place, x_lo=flip, x_hi=1 - place["x_hi"]), xo=device_at(place, x_lo=flip),
        partner=device_at(place, core=1 - place["core"]),
    )


def meet(devices):
    barrier = pltpu.get_barrier_semaphore()
    for d in devices:
        pl.semaphore_signal(barrier, inc=1, device_id=d, device_id_type=MESH)
    pl.semaphore_wait(barrier, len(devices))


ORDER = (
    ("A", -1, "0"), ("A", 1, "0"), ("X", 0, "u"), ("A", -1, "1"), ("A", 1, "1"), ("B", -1, "0"), ("D", 0, "u"),
    ("A", -2, "0"), ("A", 2, "0"), ("X", 0, "o"), ("B", -1, "1"), ("B", 1, "0"), ("X", -1, "u"), ("A", -2, "1"),
    ("A", 2, "1"), ("D", 0, "o"), ("B", -2, "0"), ("B", 1, "1"), ("X", 1, "u"), ("A", -3, "0"), ("A", 3, "0"),
    ("C", 0, ""), ("X", -1, "o"), ("B", -2, "1"), ("B", 2, "0"), ("X", -2, "u"), ("A", -3, "1"), ("A", 3, "1"),
    ("X", 1, "o"), ("B", 2, "1"), ("D", -1, "u"), ("X", 2, "u"), ("A", 4, "0"), ("X", -2, "o"), ("A", 4, "1"),
    ("D", -2, "u"), ("D", -1, "o"), ("D", 1, "u"), ("X", 2, "o"), ("C", -1, ""), ("B", -3, "0"), ("B", -3, "1"),
    ("X", -3, "u"), ("D", -2, "o"), ("B", 3, "0"), ("B", 3, "1"), ("X", 3, "u"), ("X", -3, "o"), ("C", -2, ""),
    ("B", 4, "0"), ("D", 1, "o"), ("D", 2, "u"), ("X", 3, "o"), ("B", 4, "1"), ("D", -3, "u"), ("X", 4, "u"),
    ("D", -3, "o"), ("D", 3, "u"), ("C", 1, ""), ("D", 2, "o"), ("D", 4, "u"), ("C", -3, ""), ("D", 3, "o"),
    ("X", 4, "o"), ("C", 2, ""), ("C", 3, ""), ("D", 4, "o"), ("C", 4, ""),
)


def gather_kernel(wx_ref, rest_ref, tokens_ref, inner_ref, bc_ref, dt_ref,
                  held, cut, total, own_sem, send_sem, in_sem, side_sem, shard_sem):
    place = place_of()
    near = neighbours(place)
    core, x_lo, x_hi, z, y = (place[k] for k in ("core", "x_lo", "x_hi", "z", "y"))
    me = place["seq"]
    quarter = held.shape[3]
    y_lo = lax.rem(y, 2)
    depth = cut.shape[2]
    width = wx_ref.shape[1]

    loads = [pltpu.make_async_copy(wx_ref.at[:, pl.ds(q * quarter, quarter)], held.at[q, me], own_sem.at[q]) for q in range(3)]
    tail = width - 3 * quarter
    loads.append(pltpu.make_async_copy(wx_ref.at[:, pl.ds(3 * quarter, tail)], held.at[3, me, :, pl.ds(0, tail)], own_sem.at[3]))
    loads.append(pltpu.make_async_copy(rest_ref, held.at[3, me, :, pl.ds(tail, quarter - tail)], own_sem.at[4]))
    for c in loads:
        c.start()
    meet(list(near.values()))
    for c in loads:
        c.wait()

    sent = []

    def unit(cls, dz, r):
        q = core * 2 + (y_lo if cls in "AX" else 1 - y_lo)
        xh = x_hi if cls in "AB" else 1 - x_hi
        return held.at[q, lax.rem(z + dz + ZS, ZS) * 4 + xh * 2 + r]

    def index(cls, dz, r):
        return CLASSES[cls] * 16 + (dz % ZS) * 2 + r

    def send(cls, dz, r, device, as_cls, as_dz, sem):
        ref = unit(cls, dz, r)
        c = pltpu.make_async_remote_copy(
            src_ref=ref, dst_ref=ref, send_sem=send_sem.at[len(sent)], recv_sem=sem.at[index(as_cls, as_dz, r)],
            device_id=device, device_id_type=MESH)
        c.start()
        sent.append(c)

    def arrive(cls, dz, r):
        ref = unit(cls, dz, r)
        pltpu.make_async_remote_copy(
            src_ref=ref, dst_ref=ref, send_sem=send_sem.at[0], recv_sem=in_sem.at[index(cls, dz, r)],
            device_id=near["partner"], device_id_type=MESH).wait_recv()

    def aside(cls, dz, r):
        send(cls, dz, r, near["partner"], cls, dz, side_sem)

    def along_y(r):
        return device_at(place, y=lax.rem(y + 5 - 2 * r, 4))

    shard = held.at[:, me]
    shard_copy = pltpu.make_async_remote_copy(
        src_ref=shard, dst_ref=shard, send_sem=shard_sem.at[0], recv_sem=shard_sem.at[1],
        device_id=near["partner"], device_id_type=MESH)
    shard_copy.start()
    r_u, r_o = x_lo, 1 - x_lo
    send("A", 0, core, near["zp"], "A", -1, in_sem)
    send("A", 0, core, near["zm"], "A", 1, in_sem)

    for i in range(ZS):
        cut[i] = tokens_ref[:, i * depth:(i + 1) * depth]
    total[...] = jnp.zeros_like(total)

    other = held.at[:, me + 1 - 2 * core]
    pltpu.make_async_remote_copy(
        src_ref=other, dst_ref=other, send_sem=shard_sem.at[0], recv_sem=shard_sem.at[1],
        device_id=near["partner"], device_id_type=MESH).wait_recv()
    send("A", 0, 1 - core, near["zp"], "A", -1, in_sem)
    send("A", 0, 1 - core, near["zm"], "A", 1, in_sem)
    send("A", 0, r_o, near["xu"], "X", 0, in_sem)
    send("B", 0, r_o, near["xu"], "D", 0, in_sem)
    first = set()
    for kind, dz, which in ORDER:
        if kind != "C":
            r = {"0": 0, "1": 1, "u": r_u, "o": r_o}[which]
            arrive(kind, dz, r)
        pair_done = (kind, dz) in first
        first.add((kind, dz))
        if kind == "A":
            if dz < 0 and (dz > -3 or r == 0):
                send("A", dz, r, near["zp"], "A", dz - 1, in_sem)
            if 0 < dz < 4 and (dz < 3 or r == 1):
                send("A", dz, r, near["zm"], "A", dz + 1, in_sem)
            send("A", dz, r, near["yp" if r == 0 else "ym"], "B", dz, in_sem)
            if pair_done:
                send("A", dz, r_o, near["xu"], "X", dz, in_sem)
            aside("A", dz, r)
        elif kind == "B":
            if pair_done and dz % 2 == 0:
                send("B", dz, r_o, near["xu"], "D", dz, in_sem)
            aside("B", dz, r)
        elif kind == "X":
            if which == "u":
                send("X", dz, r, near["xo"], "X", dz, in_sem)
            if dz % 2 == 1:
                send("X", dz, r, along_y(r), "D", dz, in_sem)
            aside("X", dz, r)
        elif kind == "D":
            if which == "u" and dz % 2 == 0:
                send("D", dz, r, near["xo"], "D", dz, in_sem)
            aside("D", dz, r)
        else:
            for cls in ("AB" if dz else "") + "XD":
                for r in (0, 1):
                    q = (1 - core) * 2 + (y_lo if cls in "AX" else 1 - y_lo)
                    xh = x_hi if cls in "AB" else 1 - x_hi
                    ref = held.at[q, lax.rem(z + dz + ZS, ZS) * 4 + xh * 2 + r]
                    pltpu.make_async_remote_copy(
                        src_ref=ref, dst_ref=ref, send_sem=send_sem.at[0], recv_sem=side_sem.at[index(cls, dz, r)],
                        device_id=near["partner"], device_id_type=MESH).wait_recv()
            zq = lax.rem(z + dz + ZS, ZS)

            @pl.loop(0, 4)
            def _(q):
                block = held[q, pl.ds(zq * 4, 4)].reshape(depth, quarter)
                total[q] += dot(cut[zq], block)

    for q in range(3):
        inner_ref[:, q * quarter:(q + 1) * quarter] = total[q].astype(BF16)
    inner_ref[:, 3 * quarter:] = total[3, :, :tail].astype(BF16)
    bc_ref[...] = total[3, :, tail:tail + 256].astype(BF16)
    dt_ref[...] = total[3, :, tail + 256:tail + 384]
    shard_copy.wait_send()
    for c in sent:
        c.wait_send()


def gather_project(w_x, w_bc, w_dt, tokens):
    rows, depth = tokens.shape
    width = w_x.shape[1]
    quarter = (width + 512) // 4
    pad = jnp.zeros((w_x.shape[0], 512 - w_bc.shape[1] - w_dt.shape[1]), BF16)
    rest = jnp.concatenate([w_bc, w_dt, pad], axis=1)
    vmem = pl.BlockSpec(memory_space=pltpu.VMEM)
    hbm = pl.BlockSpec(memory_space=pltpu.HBM)
    return pl.pallas_call(
        gather_kernel,
        out_shape=(
            jax.ShapeDtypeStruct((rows, width), BF16),
            jax.ShapeDtypeStruct((rows, 256), BF16),
            jax.ShapeDtypeStruct((rows, 128), F32),
        ),
        in_specs=[hbm, hbm, vmem],
        out_specs=(vmem, vmem, vmem),
        scratch_shapes=[
            pltpu.VMEM((4, 32, w_x.shape[0], quarter), BF16),
            pltpu.VMEM((ZS, rows, depth // ZS), BF16),
            pltpu.VMEM((4, rows, quarter), F32),
            pltpu.SemaphoreType.DMA((5,)),
            pltpu.SemaphoreType.DMA((160,)),
            pltpu.SemaphoreType.DMA((64,)),
            pltpu.SemaphoreType.DMA((64,)),
            pltpu.SemaphoreType.DMA((2,)),
        ],
        compiler_params=pltpu.CompilerParams(collective_id=0, has_side_effects=True, vmem_limit_bytes=60 * 2**20),
        name="gather_project",
    )(w_x, rest, tokens)


def whole(shape):
    return pl.BlockSpec(shape, lambda j: (0,) * len(shape))


def local_states(dt_raw, dt_bias, decay_rate, used, b_proj, inner):
    rows, width = inner.shape
    state_size = b_proj.shape[1]
    steps = width // WIDE
    chunks = rows // CHUNK
    pad = 128 - dt_bias.shape[0]
    bias = jnp.pad(dt_bias, (0, pad))[None]
    rate = jnp.pad(decay_rate, (0, pad))[None]
    columns = lambda r: pl.BlockSpec((r, WIDE), lambda j: (0, j))
    return pl.pallas_call(
        state_kernel,
        grid=(steps,),
        out_shape=(
            jax.ShapeDtypeStruct((chunks - 1, state_size, width), F32),
            jax.ShapeDtypeStruct((width // CHUNK, state_size, CHUNK), BF16),
            jax.ShapeDtypeStruct((width // CHUNK, CHUNK), F32),
            jax.ShapeDtypeStruct((8, width), F32),
            jax.ShapeDtypeStruct((rows, 2 * CHUNK), BF16),
            jax.ShapeDtypeStruct((steps, 4, rows), F32),
        ),
        in_specs=[
            whole((rows, 128)), whole((1, 128)), whole((1, 128)),
            pl.BlockSpec(memory_space=pltpu.SMEM),
            whole((rows, state_size)), columns(rows),
        ],
        out_specs=(
            pl.BlockSpec((chunks - 1, state_size, WIDE), lambda j: (0, 0, j)),
            pl.BlockSpec((WIDE // CHUNK, state_size, CHUNK), lambda j: (j, 0, 0)), whole((width // CHUNK, CHUNK)),
            columns(8), whole((rows, 2 * CHUNK)), whole((steps, 4, rows)),
        ),
        scratch_shapes=[
            pltpu.VMEM((rows, CHUNK), BF16),
            pltpu.VMEM((16, 2 * CHUNK), BF16),
            pltpu.VMEM((chunks, state_size, CHUNK), BF16),
        ],
        name="states",
    )(dt_raw, bias, rate, used, b_proj, inner)


def local_outputs(cum, row, c_proj, b_proj, tokens, inner, cot, gain, prior, pre, entering):
    rows, width = inner.shape
    depth = tokens.shape[1]
    state_size = b_proj.shape[1]
    steps = width // WIDE
    chunks = rows // CHUNK
    columns = lambda r: pl.BlockSpec((r, WIDE), lambda j: (0, j))
    return pl.pallas_call(
        output_kernel,
        grid=(steps,),
        out_shape=(
            jax.ShapeDtypeStruct((rows, width), BF16),
            jax.ShapeDtypeStruct((depth, state_size), BF16),
        ),
        in_specs=[
            whole((rows, 2 * CHUNK)), pl.BlockSpec((1, 4, rows), lambda j: (j, 0, 0)),
            whole((rows, state_size)), whole((rows, state_size)), whole((rows, depth)),
            columns(rows), columns(rows), columns(gain.shape[0]),
            pl.BlockSpec((chunks - 1, state_size, WIDE), lambda j: (0, 0, j)), columns(8),
            pl.BlockSpec((WIDE // CHUNK, state_size, CHUNK), lambda j: (j, 0, 0)),
        ],
        out_specs=(columns(rows), whole((depth, state_size))),
        scratch_shapes=[
            pltpu.VMEM((rows, CHUNK), F32),
            pltpu.VMEM((CHUNK, CHUNK), F32),
            pltpu.VMEM((WIDE, WIDE), BF16),
            pltpu.VMEM((rows, CHUNK), F32),
            pltpu.VMEM((rows, CHUNK), F32),
        ],
        name="outputs",
    )(cum, row, c_proj, b_proj, tokens, inner, cot, gain, prior, pre, entering)


def remote(src, dst, send_sem, recv_sem, device):
    return pltpu.make_async_remote_copy(
        src_ref=src, dst_ref=dst, send_sem=send_sem, recv_sem=recv_sem, device_id=device, device_id_type=MESH)


def exchange_kernel(state_ref, decay_ref, enter_ref, decays, paired, across, own, arrived, leaving, gone, entry,
                    d_send, d_recv, p_send, p_recv, x_send, x_recv, z_send, z_recv, e_send, e_recv):
    place = place_of()
    core, x_hi, z = place["core"], place["x_hi"], place["z"]
    partner = device_at(place, core=1 - core)
    column = device_at(place, x_hi=1 - x_hi)
    corner = device_at(place, x_hi=1 - x_hi, core=1 - core)
    up = device_at(place, z=lax.rem(z + 1, ZS))
    down = device_at(place, z=lax.rem(z + ZS - 1, ZS))
    half = state_ref.shape[0] // 2
    mine, theirs = core * half, (1 - core) * half
    member = x_hi * 2 + core

    meet([partner, column, corner, up, down])
    to_quad = [remote(decay_ref, decays.at[member], d_send.at[i], d_recv.at[i], d)
               for i, d in enumerate((partner, column, corner))]
    to_quad[0].start()
    for i in range(half):
        remote(state_ref.at[theirs + i], paired.at[i], p_send.at[i], p_recv.at[i], partner).start()
    to_quad[1].start()
    to_quad[2].start()
    decays[member] = decay_ref[...]

    @pl.when(z == 0)
    def _():
        arrived[...] = jnp.zeros_like(arrived)

    for c, i in zip(to_quad, range(3)):
        remote(decay_ref, decays.at[(member ^ (1, 2, 3)[i])], d_send.at[i], d_recv.at[i], partner).wait_recv()

    def both_cores(i):
        remote(paired.at[i], paired.at[i], p_send.at[i], p_recv.at[i], partner).wait_recv()

    @pl.loop(0, half)
    def _(i):
        both_cores(i)
        at = mine + i
        own_state, other_state = state_ref[at].astype(F32), paired[i].astype(F32)
        first = jnp.where(core == 0, own_state, other_state)
        second = jnp.where(core == 0, other_state, own_state)
        own[i] = (first * decays[x_hi * 2 + 1, pl.ds(at, 1), :] + second).astype(BF16)
        remote(own.at[i], across.at[i], x_send.at[i], x_recv.at[i], column).start()

    @pl.loop(0, half)
    def _(i):
        at = mine + i
        d = [decays[m, pl.ds(at, 1), :] for m in range(4)]
        remote(own.at[i], across.at[i], x_send.at[i], x_recv.at[i], column).wait_recv()
        mine_t, other_t = own[i].astype(F32), across[i].astype(F32)
        t0 = jnp.where(x_hi == 0, mine_t, other_t)
        t1 = jnp.where(x_hi == 0, other_t, mine_t)
        d0, d1 = d[0] * d[1], d[2] * d[3]

        @pl.when(z > 0)
        def _():
            remote(arrived.at[i], arrived.at[i], z_send.at[i], z_recv.at[i], down).wait_recv()

        before = arrived[i].astype(F32)

        @pl.when(z < ZS - 1)
        def _():
            leaving[i] = (before * (d0 * d1) + (t0 * d1 + t1)).astype(BF16)
            remote(leaving.at[i], arrived.at[i], z_send.at[i], z_recv.at[i], up).start()

        here = jnp.where(x_hi == 0, before, before * d0 + t0)
        first = jnp.where(core == 0, state_ref[at].astype(F32), paired[i].astype(F32))
        after = here * jnp.where(x_hi == 0, d[0], d[2]) + first
        entry[at] = jnp.where(core == 0, here, after).astype(BF16)
        gone[i] = jnp.where(core == 0, after, here).astype(BF16)
        remote(gone.at[i], entry.at[at], e_send.at[i], e_recv.at[i], partner).start()

    @pl.loop(0, half)
    def _(i):
        remote(gone.at[i], entry.at[theirs + i], e_send.at[i], e_recv.at[i], partner).wait_recv()
        remote(gone.at[i], entry.at[theirs + i], e_send.at[i], e_recv.at[i], partner).wait_send()
        remote(own.at[i], across.at[i], x_send.at[i], x_recv.at[i], column).wait_send()
        remote(paired.at[i], paired.at[i], p_send.at[i], p_recv.at[i], partner).wait_send()

        @pl.when(z < ZS - 1)
        def _():
            remote(leaving.at[i], arrived.at[i], z_send.at[i], z_recv.at[i], up).wait_send()

    for c in to_quad:
        c.wait_send()
    enter_ref[...] = entry[...]


def entering_states(state, decay):
    tiles = state.shape[0]
    tile = state.shape[1:]
    half = tiles // 2
    vmem = pl.BlockSpec(memory_space=pltpu.VMEM)
    sems = pltpu.SemaphoreType.DMA
    return pl.pallas_call(
        exchange_kernel,
        out_shape=jax.ShapeDtypeStruct(state.shape, BF16),
        in_specs=[vmem, vmem],
        out_specs=vmem,
        scratch_shapes=[pltpu.VMEM((4,) + decay.shape, F32)]
        + [pltpu.VMEM((half,) + tile, BF16)] * 6
        + [pltpu.VMEM(state.shape, BF16)]
        + [sems((3,))] * 2 + [sems((half,))] * 8,
        compiler_params=pltpu.CompilerParams(collective_id=1, has_side_effects=True),
        name="entering_states",
    )(state, decay)


def reduce_kernel(part_ref, out_ref, paired, held, landed, own, copies, a_send, a_recv, b_send, b_recv, c_send, c_recv):
    place = place_of()
    core, dp = place["core"], place["dp"]
    peers, parts = held.shape[0], copies.shape[0]
    here = place["seq"] // 2
    partner = device_at(place, core=1 - core)

    def in_column(o):
        b = lax.rem(here + o, peers)
        return b, (dp, b * 2 + core)

    def in_dp(o):
        return (lax.rem(dp + o, parts), place["seq"])

    meet([partner] + [in_column(o)[1] for o in range(1, peers)] + [in_dp(o) for o in range(1, parts)])
    first = remote(part_ref.at[1 - core], paired, a_send, a_recv, partner)
    first.start()
    first.wait()
    held[...] = (part_ref[core].astype(F32) + paired[...].astype(F32)).astype(BF16)
    sent = []
    for o in range(1, peers):
        b, device = in_column(o)
        c = remote(held.at[b], landed.at[o - 1], b_send.at[o - 1], b_recv.at[o - 1], device)
        c.start()
        sent.append(c)
    total = held[here].astype(F32)
    for o in range(1, peers):
        sent[o - 1].wait_recv()
        total = total + landed[o - 1].astype(F32)
    own[...] = total.astype(BF16)
    copies[dp] = own[...]
    given = []
    for o in range(1, parts):
        c = remote(own, copies.at[dp], c_send.at[o - 1], c_recv.at[o - 1], in_dp(o))
        c.start()
        given.append(c)
    for o in range(1, parts):
        source = lax.rem(dp + parts - o, parts)
        remote(own, copies.at[source], c_send.at[o - 1], c_recv.at[o - 1], in_dp(o)).wait_recv()
    total = copies[0].astype(F32)
    for i in range(1, parts):
        total = total + copies[i].astype(F32)
    out_ref[...] = total
    for c in sent + given:
        c.wait_send()


def reduced_gradient(grad):
    block = grad.shape[2:]
    peers, parts = grad.shape[1], 8
    vmem = pl.BlockSpec(memory_space=pltpu.VMEM)
    sems = pltpu.SemaphoreType.DMA
    return pl.pallas_call(
        reduce_kernel,
        out_shape=jax.ShapeDtypeStruct(block, F32),
        in_specs=[vmem],
        out_specs=vmem,
        scratch_shapes=[
            pltpu.VMEM((peers,) + block, BF16), pltpu.VMEM((peers,) + block, BF16),
            pltpu.VMEM((peers - 1,) + block, BF16), pltpu.VMEM(block, BF16), pltpu.VMEM((parts,) + block, BF16),
            sems, sems, sems((peers - 1,)), sems((peers - 1,)), sems((parts - 1,)), sems((parts - 1,)),
        ],
        compiler_params=pltpu.CompilerParams(collective_id=2, has_side_effects=True),
        name="reduced_gradient",
    )(grad)


def body(tokens, w_x, w_bc, w_dt, dt_bias, decay_rate, gain, cotangent, counts):
    seq_tokens = tokens[0]
    cot_rows = cotangent[0]
    slot_count = seq_tokens.shape[0] // L
    state_size = w_bc.shape[1] // 2
    group_index = lax.axis_index("seq")
    filled = jnp.sum(jnp.where(jnp.arange(counts.shape[0]) == group_index, counts, 0))
    slot_used = (jnp.arange(slot_count) < filled).astype(F32)
    inner, bc_raw, dt_raw = gather_project(w_x, w_bc, w_dt, seq_tokens)
    b_proj, c_proj = bc_raw[:, :state_size], bc_raw[:, state_size:]
    prior, total, decay, pre, cum, row = local_states(dt_raw, dt_bias, decay_rate, slot_used[None], b_proj, inner)
    entering = entering_states(total, decay)
    gains = gain[None] * slot_used[:, None]
    outputs, grad = local_outputs(cum, row, c_proj, b_proj, seq_tokens, inner, cot_rows, gains, prior, pre, entering)
    rows = grad.shape[0] // 32
    gradient = reduced_gradient(jnp.swapaxes(grad.reshape(16, 2, rows, state_size), 0, 1))
    return (outputs[None], gradient)


def solution(mesh):
    return jax.shard_map(
        body,
        mesh=mesh,
        in_specs=(
            P("dp", "seq", None), P("seq", None), P("seq", None), P("seq", None),
            P(), P(), P(), P("dp", "seq", None), P(),
        ),
        out_specs=(P("dp", "seq", None), P("seq", None)),
        check_vma=False,
    )
```

```python
import functools

import jax
import jax.numpy as jnp
from jax import lax
from jax.experimental import pallas as pl
from jax.experimental.pallas import tpu as pltpu
from jax.sharding import Mesh
from jax.sharding import PartitionSpec as P

L = 256
CHUNK = 128
WIDE = 256
LOG2E = 1.4426950408889634
F32 = jnp.float32
BF16 = jnp.bfloat16


def dot(a, b):
    return jnp.dot(a, b, preferred_element_type=F32)


def dot_lanes(a, b):
    return lax.dot_general(a, b, (((1,), (1,)), ((), ())), preferred_element_type=F32)


def iota(shape, dim):
    return lax.broadcasted_iota(jnp.int32, shape, dim)


def split3(x):
    hi = x.astype(BF16).astype(F32)
    mid = (x - hi).astype(BF16).astype(F32)
    return hi, mid, x - hi - mid


def packed3(x):
    hi, mid, lo = split3(x)
    low_lanes = iota(x.shape, 1) < 64
    first = jnp.where(low_lanes, hi, pltpu.roll(mid, 64, 1))
    second = jnp.where(low_lanes, lo, 0.0)
    return jnp.concatenate([first.astype(BF16), second.astype(BF16)], axis=1)


def head_select(depth, first_head, lanes_per_head, lanes=WIDE):
    k = iota((depth, lanes), 0)
    l = iota((depth, lanes), 1)
    hit = ((k & 63) == first_head + l // lanes_per_head) & (k < 192)
    return jnp.where(hit, 1.0, 0.0).astype(BF16)


def slots_used(counts_ref):
    filled = counts_ref[lax.axis_index("seq")]
    return [jnp.where(filled > k, 1.0, 0.0).astype(F32) for k in range(2)]


def decay_kernel(dt_ref, bias_ref, rate_ref, counts_ref, b_ref,
                 cum_ref, row_ref, to_end, b_turned, pre_ref, decay_ref, ends, padded):
    rows = dt_ref.shape[0]
    chunks = rows // CHUNK
    heads = bias_ref.shape[1]
    padded[...] = jnp.zeros_like(padded)
    padded[0:1, :heads] = bias_ref[...]
    padded[1:2, :heads] = rate_ref[...]
    used = slots_used(counts_ref)
    v = dt_ref[...] + padded[0:1, :]
    dt = jnp.maximum(v, 0.0) + jnp.log1p(jnp.exp(-jnp.abs(v)))
    slot = iota(dt.shape, 0) // L
    dt = dt * jnp.where(slot == 0, used[0], used[1])
    drop = dt * (padded[1:2, :] * (-LOG2E))
    tri = jnp.where(iota((CHUNK, CHUNK), 0) >= iota((CHUNK, CHUNK), 1), 1.0, 0.0).astype(BF16)
    lasts = []
    for c in range(chunks):
        at = slice(c * CHUNK, (c + 1) * CHUNK)
        hi, mid, lo = split3(drop[at])
        cum = dot(tri, hi.astype(BF16)) + dot(tri, mid.astype(BF16)) + dot(tri, lo.astype(BF16))
        own = cum - jnp.log2(dt[at])
        last = cum[CHUNK - 1:CHUNK]
        lasts.append(last)
        cum_ref[at, :] = packed3(cum)
        reach = jnp.exp2(last - own)
        reach_hi = reach.astype(BF16).astype(F32)
        reach_lo = pltpu.roll(reach - reach_hi, 64, 1)
        to_end[at, :] = jnp.where(iota(reach.shape, 1) < 64, reach_hi, reach_lo).astype(BF16)
        turned = own.T
        for g in range(row_ref.shape[0]):
            row_ref[g, :, at] = turned[2 * g:2 * g + 2]
        b_turned[c] = b_ref[at, :].astype(F32).T.astype(BF16)
    lasts = jnp.concatenate(lasts + [jnp.zeros((16 - chunks, CHUNK), F32)], axis=0)
    ends[...] = packed3(lasts)

    @pl.loop(0, pre_ref.shape[0])
    def _(j):
        decay = jnp.exp2(dot(ends[...], head_select(2 * CHUNK, 2 * j, 64, CHUNK)))
        before = jnp.ones((1, CHUNK), F32)
        for c in range(chunks):
            pre_ref[j, c:c + 1, :] = before
            before = before * decay[c:c + 1]
        pre_ref[j, chunks:2 * chunks, :] = decay[:chunks]
        decay_ref[pl.ds(j, 1), :] = before


def output_kernel(cum_ref, c_ref, b_ref, counts_ref, tokens_ref, inner_ref, cot_ref, gain_ref, intra_ref, weight_ref,
                  prior_ref, pre_ref, enter_ref, out_ref, grad_ref, sum_heads, combined, through, full_grad):
    step = pl.program_id(0)
    rows = c_ref.shape[0]
    chunks = rows // CHUNK

    @pl.when(step == 0)
    def _():
        same = iota(sum_heads.shape, 0) // 64 == iota(sum_heads.shape, 1) // 64
        sum_heads[...] = jnp.where(same, 1.0, 0.0).astype(BF16)
        combined[...] = jnp.zeros_like(combined)
        through[...] = jnp.zeros_like(through)

    used = slots_used(counts_ref)
    low_half = iota((CHUNK, CHUNK), 1) < 64
    growths = jnp.exp2(dot(cum_ref[...], head_select(2 * CHUNK, step * 4, 64)))
    entry = jnp.concatenate([enter_ref[p].astype(F32) for p in range(2)], axis=1)
    for c in range(chunks):
        at = slice(c * CHUNK, (c + 1) * CHUNK)
        entering = entry * jnp.concatenate([pre_ref[p, c:c + 1, :] for p in range(2)], axis=1)
        if c > 0:
            entering = entering + jnp.concatenate([prior_ref[p, c - 1] for p in range(2)], axis=1)
        state_low = entering.astype(BF16)
        from_state = dot(c_ref[at, :], state_low) * growths[at]
        gain_row = gain_ref[...] * used[c * CHUNK // L]
        scaled = []
        for p in range(2):
            lanes = slice(p * CHUNK, (p + 1) * CHUNK)
            x = inner_ref[at, lanes]
            zero = jnp.zeros_like(x)
            heads = jnp.concatenate([jnp.where(low_half, x, zero), jnp.where(low_half, zero, x)], axis=0)
            full = intra_ref[p, at, :] + from_state[:, lanes]
            gain = gain_row[:, lanes]
            grad_out = cot_ref[at, lanes].astype(F32) * gain
            parts = jnp.concatenate([(full * full).astype(BF16), (grad_out * full).astype(BF16)], axis=1)
            sums = dot(parts, sum_heads[...])
            inverse = lax.rsqrt(sums[:, :CHUNK] * (1.0 / 64) + 1.0)
            normed = full * inverse
            out_ref[at, lanes] = (normed * gain).astype(BF16)
            grad = inverse * (grad_out - normed * (sums[:, CHUNK:] * inverse * (1.0 / 64)))
            inter = dot_lanes(grad.astype(BF16), heads) * weight_ref[p, at, :].astype(F32)
            combined[at, :] += inter[:, :CHUNK] + inter[:, CHUNK:]
            scaled.append((grad * growths[at, lanes]).astype(BF16))
        through[at, :] += dot_lanes(jnp.concatenate(scaled, axis=1), state_low)

    @pl.when(step == pl.num_programs(0) - 1)
    def _():
        turned = []
        for c in range(chunks):
            at = slice(c * CHUNK, (c + 1) * CHUNK)
            grad_rows = dot(combined[at, :].astype(BF16), b_ref[at, :]) + through[at, :]
            turned.append(grad_rows.astype(BF16).astype(F32).T.astype(BF16))
        turned = jnp.concatenate(turned, axis=1)
        for k in range(full_grad.shape[0] // CHUNK):
            at = slice(k * CHUNK, (k + 1) * CHUNK)
            full_grad[at, :] = dot(turned, tokens_ref[:, at]).T.astype(BF16)
        block = grad_ref.shape[2]
        for k in range(full_grad.shape[0] // block):
            grad_ref[k % 2, k // 2] = full_grad[k * block:(k + 1) * block, :]


MESH = pl.DeviceIdType.MESH
ZS = 8
CLASSES = {"A": 0, "B": 1, "X": 2, "D": 3}


def place_of():
    dp, seq = lax.axis_index("dp"), lax.axis_index("seq")
    return dict(y=dp // 2, x_lo=lax.rem(dp, 2), z=seq // 4, x_hi=lax.rem(seq // 2, 2), core=lax.rem(seq, 2), seq=seq, dp=dp)


def device_at(place, **new):
    p = {**place, **new}
    return (p["y"] * 2 + p["x_lo"], p["z"] * 4 + p["x_hi"] * 2 + p["core"])


def neighbours(place):
    z, y = place["z"], place["y"]
    flip = 1 - place["x_lo"]
    return dict(
        zp=device_at(place, z=lax.rem(z + 1, ZS)), zm=device_at(place, z=lax.rem(z + ZS - 1, ZS)),
        yp=device_at(place, y=lax.rem(y + 1, 4)), ym=device_at(place, y=lax.rem(y + 3, 4)),
        xu=device_at(place, x_lo=flip, x_hi=1 - place["x_hi"]), xo=device_at(place, x_lo=flip),
        partner=device_at(place, core=1 - place["core"]),
    )


def meet(devices):
    barrier = pltpu.get_barrier_semaphore()
    for d in devices:
        pl.semaphore_signal(barrier, inc=1, device_id=d, device_id_type=MESH)
    pl.semaphore_wait(barrier, len(devices))


ORDER = (
    ("A", -1, "0"), ("A", 1, "0"), ("A", -1, "1"), ("A", 1, "1"), ("X", 0, "u"), ("B", -1, "0"), ("A", -2, "0"),
    ("A", 2, "0"), ("D", 0, "u"), ("B", 1, "0"), ("B", -1, "1"), ("X", 0, "o"), ("A", -2, "1"), ("A", 2, "1"),
    ("X", -1, "u"), ("B", -2, "0"), ("B", 1, "1"), ("D", 0, "o"), ("A", -3, "0"), ("A", 3, "0"), ("X", 1, "u"),
    ("B", -2, "1"), ("B", 2, "0"), ("X", -1, "o"), ("C", 0, ""), ("A", -3, "1"), ("A", 3, "1"), ("X", -2, "u"),
    ("B", 2, "1"), ("D", -1, "u"), ("X", 1, "o"), ("A", 4, "0"), ("X", 2, "u"), ("B", -3, "0"), ("D", -1, "o"),
    ("A", 4, "1"), ("X", -3, "u"), ("X", -2, "o"), ("C", -1, ""), ("D", -2, "u"), ("B", -3, "1"), ("B", 3, "0"),
    ("X", 2, "o"), ("X", 3, "u"), ("D", -2, "o"), ("B", 3, "1"), ("D", 1, "u"), ("X", -3, "o"), ("X", 4, "u"),
    ("C", -2, ""), ("B", 4, "0"), ("D", 1, "o"), ("D", -3, "u"), ("X", 3, "o"), ("D", 2, "u"), ("C", 1, ""),
    ("B", 4, "1"), ("D", 4, "u"), ("D", 3, "u"), ("X", 4, "o"), ("D", 2, "o"), ("D", -3, "o"), ("D", 4, "o"),
    ("C", 2, ""), ("D", 3, "o"), ("C", -3, ""), ("C", 4, ""), ("C", 3, ""),
)
FAR = ("x", "y", "z", "x", "y")


def gather_kernel(wx_ref, wbc_ref, wdt_ref, tokens_ref, inner_ref, b_ref, c_ref, dt_ref,
                  held, cut, total, own_sem, send_sem, in_sem, side_sem, shard_sem):
    place = place_of()
    near = neighbours(place)
    core, x_lo, x_hi, z, y = (place[k] for k in ("core", "x_lo", "x_hi", "z", "y"))
    me = place["seq"]
    quarter = held.shape[3]
    y_lo = lax.rem(y, 2)
    depth = cut.shape[2]
    width = wx_ref.shape[1]

    loads = [pltpu.make_async_copy(wx_ref.at[:, pl.ds(q * quarter, quarter)], held.at[q, me], own_sem.at[q]) for q in range(3)]
    tail = width - 3 * quarter
    loads.append(pltpu.make_async_copy(wx_ref.at[:, pl.ds(3 * quarter, tail)], held.at[3, me, :, pl.ds(0, tail)], own_sem.at[3]))
    loads.append(pltpu.make_async_copy(wbc_ref, held.at[3, me, :, pl.ds(tail, wbc_ref.shape[1])], own_sem.at[4]))
    for c in loads:
        c.start()
    spare = quarter - tail - wbc_ref.shape[1] - wdt_ref.shape[1]
    held[3, me, :, tail + wbc_ref.shape[1]:] = jnp.concatenate(
        [wdt_ref[...].astype(F32), jnp.zeros((wdt_ref.shape[0], spare), F32)], axis=1).astype(BF16)
    meet(list(near.values()))
    for c in loads:
        c.wait()

    sent = []

    def unit(cls, dz, r):
        q = core * 2 + (y_lo if cls in "AX" else 1 - y_lo)
        xh = x_hi if cls in "AB" else 1 - x_hi
        return held.at[q, lax.rem(z + dz + ZS, ZS) * 4 + xh * 2 + r]

    def index(cls, dz, r):
        return CLASSES[cls] * 16 + (dz % ZS) * 2 + r

    def send(cls, dz, r, device, as_cls, as_dz, sem):
        ref = unit(cls, dz, r)
        c = pltpu.make_async_remote_copy(
            src_ref=ref, dst_ref=ref, send_sem=send_sem.at[len(sent)], recv_sem=sem.at[index(as_cls, as_dz, r)],
            device_id=device, device_id_type=MESH)
        c.start()
        sent.append(c)

    def arrive(cls, dz, r):
        ref = unit(cls, dz, r)
        pltpu.make_async_remote_copy(
            src_ref=ref, dst_ref=ref, send_sem=send_sem.at[0], recv_sem=in_sem.at[index(cls, dz, r)],
            device_id=near["partner"], device_id_type=MESH).wait_recv()

    def aside(cls, dz, r):
        send(cls, dz, r, near["partner"], cls, dz, side_sem)

    def along_y(r):
        return device_at(place, y=lax.rem(y + 5 - 2 * r, 4))

    shard = held.at[:, me]
    shard_copy = pltpu.make_async_remote_copy(
        src_ref=shard, dst_ref=shard, send_sem=shard_sem.at[0], recv_sem=shard_sem.at[1],
        device_id=near["partner"], device_id_type=MESH)
    shard_copy.start()
    r_u, r_o = x_lo, 1 - x_lo
    send("A", 0, core, near["zp"], "A", -1, in_sem)
    send("A", 0, core, near["zm"], "A", 1, in_sem)

    for i in range(ZS):
        cut[i] = tokens_ref[:, i * depth:(i + 1) * depth]
    total[...] = jnp.zeros_like(total)

    other = held.at[:, me + 1 - 2 * core]
    pltpu.make_async_remote_copy(
        src_ref=other, dst_ref=other, send_sem=shard_sem.at[0], recv_sem=shard_sem.at[1],
        device_id=near["partner"], device_id_type=MESH).wait_recv()
    send("A", 0, 1 - core, near["zp"], "A", -1, in_sem)
    send("A", 0, 1 - core, near["zm"], "A", 1, in_sem)
    send("A", 0, r_o, near["xu"], "X", 0, in_sem)
    send("B", 0, r_o, near["xu"], "D", 0, in_sem)
    first = set()
    for kind, dz, which in ORDER:
        if kind != "C":
            r = {"0": 0, "1": 1, "u": r_u, "o": r_o}[which]
            arrive(kind, dz, r)
        pair_done = (kind, dz) in first
        first.add((kind, dz))
        if kind == "A":
            if dz < 0 and (dz > -3 or r == 0):
                send("A", dz, r, near["zp"], "A", dz - 1, in_sem)
            if 0 < dz < 4 and (dz < 3 or r == 1):
                send("A", dz, r, near["zm"], "A", dz + 1, in_sem)
            send("A", dz, r, near["yp" if r == 0 else "ym"], "B", dz, in_sem)
            if pair_done:
                send("A", dz, r_o, near["xu"], "X", dz, in_sem)
            aside("A", dz, r)
        elif kind == "B":
            if pair_done and FAR[abs(dz)] == "x":
                send("B", dz, r_o, near["xu"], "D", dz, in_sem)
            aside("B", dz, r)
        elif kind == "X":
            if which == "u":
                send("X", dz, r, near["xo"], "X", dz, in_sem)
            if FAR[abs(dz)] == "y":
                send("X", dz, r, along_y(r), "D", dz, in_sem)
            aside("X", dz, r)
        elif kind == "D":
            if which == "u" and FAR[abs(dz)] == "x":
                send("D", dz, r, near["xo"], "D", dz, in_sem)
            if -3 < dz <= 0 and FAR[abs(dz) + 1] == "z":
                send("D", dz, r, near["zp"], "D", dz - 1, in_sem)
            if 0 <= dz < 3 and FAR[abs(dz) + 1] == "z":
                send("D", dz, r, near["zm"], "D", dz + 1, in_sem)
            aside("D", dz, r)
        else:
            for cls in ("AB" if dz else "") + "XD":
                for r in (0, 1):
                    q = (1 - core) * 2 + (y_lo if cls in "AX" else 1 - y_lo)
                    xh = x_hi if cls in "AB" else 1 - x_hi
                    ref = held.at[q, lax.rem(z + dz + ZS, ZS) * 4 + xh * 2 + r]
                    pltpu.make_async_remote_copy(
                        src_ref=ref, dst_ref=ref, send_sem=send_sem.at[0], recv_sem=side_sem.at[index(cls, dz, r)],
                        device_id=near["partner"], device_id_type=MESH).wait_recv()
            zq = lax.rem(z + dz + ZS, ZS)

            @pl.loop(0, 4)
            def _(q):
                block = held[q, pl.ds(zq * 4, 4)].reshape(depth, quarter)
                total[q] += dot(cut[zq], block)

    for q in range(3):
        inner_ref[:, q * quarter:(q + 1) * quarter] = total[q].astype(BF16)
    inner_ref[:, 3 * quarter:] = total[3, :, :tail].astype(BF16)
    b_ref[...] = total[3, :, tail:tail + 128].astype(BF16)
    c_ref[...] = total[3, :, tail + 128:tail + 256].astype(BF16)
    dt_ref[...] = total[3, :, tail + 256:tail + 384]
    shard_copy.wait_send()
    for c in sent:
        c.wait_send()


def gather_project(w_x, w_bc, w_dt, tokens):
    rows, depth = tokens.shape
    width = w_x.shape[1]
    quarter = (width + 512) // 4
    vmem = pl.BlockSpec(memory_space=pltpu.VMEM)
    hbm = pl.BlockSpec(memory_space=pltpu.HBM)
    return pl.pallas_call(
        gather_kernel,
        out_shape=(
            jax.ShapeDtypeStruct((rows, width), BF16),
            jax.ShapeDtypeStruct((rows, 128), BF16),
            jax.ShapeDtypeStruct((rows, 128), BF16),
            jax.ShapeDtypeStruct((rows, 128), F32),
        ),
        in_specs=[hbm, hbm, vmem, vmem],
        out_specs=(vmem,) * 4,
        scratch_shapes=[
            pltpu.VMEM((4, 32, w_x.shape[0], quarter), BF16),
            pltpu.VMEM((ZS, rows, depth // ZS), BF16),
            pltpu.VMEM((4, rows, quarter), F32),
            pltpu.SemaphoreType.DMA((5,)),
            pltpu.SemaphoreType.DMA((160,)),
            pltpu.SemaphoreType.DMA((64,)),
            pltpu.SemaphoreType.DMA((64,)),
            pltpu.SemaphoreType.DMA((2,)),
        ],
        compiler_params=pltpu.CompilerParams(collective_id=0, has_side_effects=True, vmem_limit_bytes=67043328),
        name="gather_project",
    )(w_x, w_bc, w_dt, tokens)


def whole(shape):
    return pl.BlockSpec(shape, lambda j: (0,) * len(shape))


def local_decays(dt_raw, dt_bias, decay_rate, counts, b_proj, tiles):
    rows, state_size = b_proj.shape
    chunks = rows // CHUNK
    vmem = pl.BlockSpec(memory_space=pltpu.VMEM)
    return pl.pallas_call(
        decay_kernel,
        out_shape=(
            jax.ShapeDtypeStruct((rows, 2 * CHUNK), BF16),
            jax.ShapeDtypeStruct((tiles, 2, rows), F32),
            jax.ShapeDtypeStruct((rows, CHUNK), BF16),
            jax.ShapeDtypeStruct((chunks, state_size, CHUNK), BF16),
            jax.ShapeDtypeStruct((tiles, 2 * chunks, CHUNK), F32),
            jax.ShapeDtypeStruct((tiles, CHUNK), F32),
        ),
        in_specs=[vmem, vmem, vmem, pl.BlockSpec(memory_space=pltpu.SMEM), vmem],
        out_specs=(vmem,) * 6,
        scratch_shapes=[pltpu.VMEM((16, 2 * CHUNK), BF16), pltpu.VMEM((8, 128), F32)],
        name="decays",
    )(dt_raw, dt_bias[None], decay_rate[None], counts, b_proj)


def local_outputs(cum, c_proj, b_proj, counts, tokens, inner, cot, gain, intra, weight, prior, pre, entering):
    rows, width = inner.shape
    depth = tokens.shape[1]
    state_size = b_proj.shape[1]
    steps = width // WIDE
    chunks = rows // CHUNK
    owners = 32
    tiles = WIDE // CHUNK
    columns = lambda r: pl.BlockSpec((r, WIDE), lambda j: (0, j))
    tiled = lambda a, b: pl.BlockSpec((tiles, a, b), lambda j: (j, 0, 0))
    grad_shape = (2, owners // 2, depth // owners, state_size)
    return pl.pallas_call(
        output_kernel,
        grid=(steps,),
        out_shape=(
            jax.ShapeDtypeStruct((rows, width), BF16),
            jax.ShapeDtypeStruct(grad_shape, BF16),
        ),
        in_specs=[
            whole((rows, 2 * CHUNK)), whole((rows, state_size)), whole((rows, state_size)),
            pl.BlockSpec(memory_space=pltpu.SMEM), whole((rows, depth)),
            columns(rows), columns(rows), columns(1), tiled(rows, CHUNK), tiled(rows, WIDE),
            pl.BlockSpec((tiles, chunks - 1, state_size, CHUNK), lambda j: (j, 0, 0, 0)),
            tiled(2 * chunks, CHUNK), tiled(state_size, CHUNK),
        ],
        out_specs=(columns(rows), whole(grad_shape)),
        scratch_shapes=[
            pltpu.VMEM((WIDE, WIDE), BF16),
            pltpu.VMEM((rows, CHUNK), F32),
            pltpu.VMEM((rows, CHUNK), F32),
            pltpu.VMEM((depth, state_size), BF16),
        ],
        name="outputs",
    )(cum, c_proj, b_proj, counts, tokens, inner, cot, gain[None], intra, weight, prior, pre, entering)


def remote(src, dst, send_sem, recv_sem, device):
    return pltpu.make_async_remote_copy(
        src_ref=src, dst_ref=dst, send_sem=send_sem, recv_sem=recv_sem, device_id=device, device_id_type=MESH)


AHEAD = (2, 4)


def exchange_kernel(cum_in, row_in, reach_in, turned_in, pre_in, decay_ref, c_in, b_in, inner_in,
                    enter_ref, intra_ref, weight_ref, prior_ref,
                    cum_ref, row_ref, reach_ref, turned_ref, pre_ref, c_ref, b_ref, inner_ref, load_sem,
                    state, prior, s_done,
                    decays, paired, across, own, arrived, leaving, gone, entry, intra, weight, gram, hide, y_done, w_done,
                    d_send, d_recv, p_send, p_recv, x_send, x_recv, z_send, z_recv, e_send, e_recv):
    loads = [pltpu.make_async_copy(a, b, load_sem.at[i]) for i, (a, b) in enumerate((
        (inner_in, inner_ref), (reach_in, reach_ref), (turned_in, turned_ref), (pre_in, pre_ref),
        (cum_in, cum_ref), (row_in, row_ref), (c_in, c_ref), (b_in, b_ref)))]
    for c in loads:
        c.start()
    place = place_of()
    core, x_hi, z = place["core"], place["x_hi"], place["z"]
    partner = device_at(place, core=1 - core)
    column = device_at(place, x_hi=1 - x_hi)
    corner = device_at(place, x_hi=1 - x_hi, core=1 - core)
    up = device_at(place, z=lax.rem(z + 1, ZS))
    down = device_at(place, z=lax.rem(z + ZS - 1, ZS))
    half = state.shape[0] // 2
    chunks = prior.shape[1] + 1
    mine, theirs = core * half, (1 - core) * half
    member = x_hi * 2 + core

    meet([partner, column, corner, up, down])
    to_quad = [remote(decay_ref, decays.at[member], d_send.at[i], d_recv.at[i], d)
               for i, d in enumerate((partner, column, corner))]
    to_quad[0].start()
    to_quad[1].start()
    to_quad[2].start()
    for c in loads:
        c.wait()

    def pair_of(j):
        return inner_ref[:, pl.ds(pl.multiple_of(j * CHUNK, CHUNK), CHUNK)]

    def added(j):
        reach = dot(reach_ref[...], head_select(CHUNK, 2 * j, 64, CHUNK))
        scaled = (pair_of(j).astype(F32) * reach).astype(BF16)
        now = dot(turned_ref[0], scaled[:CHUNK])
        for c in range(1, chunks):
            prior[j, c - 1] = now
            now = now * pre_ref[j, chunks + c:chunks + c + 1, :] + dot(turned_ref[c], scaled[c * CHUNK:(c + 1) * CHUNK])
        pltpu.make_async_copy(prior.at[j], prior_ref.at[j], s_done.at[j]).start()
        state[j] = now.astype(BF16)

    @pl.loop(0, half)
    def _(i):
        added(theirs + i)
        remote(state.at[theirs + i], paired.at[i], p_send.at[i], p_recv.at[i], partner).start()

    decays[member] = decay_ref[...]

    @pl.when(z == 0)
    def _():
        arrived[...] = jnp.zeros_like(arrived)

    for c, i in zip(to_quad, range(3)):
        remote(decay_ref, decays.at[(member ^ (1, 2, 3)[i])], d_send.at[i], d_recv.at[i], partner).wait_recv()

    def both_cores(i):
        remote(paired.at[i], paired.at[i], p_send.at[i], p_recv.at[i], partner).wait_recv()

    @pl.loop(0, half)
    def _(i):
        at = mine + i
        added(at)
        both_cores(i)
        own_state, other_state = state[at].astype(F32), paired[i].astype(F32)
        first = jnp.where(core == 0, own_state, other_state)
        second = jnp.where(core == 0, other_state, own_state)
        own[i] = (first * decays[x_hi * 2 + 1, pl.ds(at, 1), :] + second).astype(BF16)
        remote(own.at[i], across.at[i], x_send.at[i], x_recv.at[i], column).start()

    for c in range(chunks):
        at = slice(c * CHUNK, (c + 1) * CHUNK)
        gram[at, :] = dot_lanes(c_ref[at, :], b_ref[at, :])
    hide[...] = jnp.where(iota(hide.shape, 0) >= iota(hide.shape, 1), 0.0, -1e30)
    tiles = intra.shape[0]

    def within(j):
        spread = dot(cum_ref[...], head_select(2 * CHUNK, 2 * j, CHUNK))
        low_half = iota((CHUNK, CHUNK), 1) < 64
        pair = pair_of(j)
        for c in range(chunks):
            at = slice(c * CHUNK, (c + 1) * CHUNK)
            w0 = jnp.exp2(spread[at, :CHUNK] - row_ref[j, 0:1, at] + hide[...])
            w1 = jnp.exp2(spread[at, CHUNK:] - row_ref[j, 1:2, at] + hide[...])
            dots = gram[at, :]
            mixing = jnp.concatenate([(dots * w0).astype(BF16), (dots * w1).astype(BF16)], axis=1)
            weight[j, at, :] = jnp.concatenate([w0.astype(BF16), w1.astype(BF16)], axis=1)
            x = pair[at]
            zero = jnp.zeros_like(x)
            heads = jnp.concatenate([jnp.where(low_half, x, zero), jnp.where(low_half, zero, x)], axis=0)
            intra[j, at, :] = dot(mixing, heads)
        pltpu.make_async_copy(intra.at[j], intra_ref.at[j], y_done.at[j]).start()
        pltpu.make_async_copy(weight.at[j], weight_ref.at[j], w_done.at[j]).start()

    ahead = jnp.minimum(AHEAD[0] + AHEAD[1] * z, tiles)
    pl.loop(0, ahead)(within)

    @pl.loop(0, half)
    def _(i):
        at = mine + i
        d = [decays[m, pl.ds(at, 1), :] for m in range(4)]
        remote(own.at[i], across.at[i], x_send.at[i], x_recv.at[i], column).wait_recv()
        mine_t, other_t = own[i].astype(F32), across[i].astype(F32)
        t0 = jnp.where(x_hi == 0, mine_t, other_t)
        t1 = jnp.where(x_hi == 0, other_t, mine_t)
        d0, d1 = d[0] * d[1], d[2] * d[3]

        @pl.when(z > 0)
        def _():
            remote(arrived.at[i], arrived.at[i], z_send.at[i], z_recv.at[i], down).wait_recv()

        before = arrived[i].astype(F32)

        @pl.when(z < ZS - 1)
        def _():
            leaving[i] = (before * (d0 * d1) + (t0 * d1 + t1)).astype(BF16)
            remote(leaving.at[i], arrived.at[i], z_send.at[i], z_recv.at[i], up).start()

        here = jnp.where(x_hi == 0, before, before * d0 + t0)
        first = jnp.where(core == 0, state[at].astype(F32), paired[i].astype(F32))
        after = here * jnp.where(x_hi == 0, d[0], d[2]) + first
        entry[at] = jnp.where(core == 0, here, after).astype(BF16)
        gone[i] = jnp.where(core == 0, after, here).astype(BF16)
        remote(gone.at[i], entry.at[at], e_send.at[i], e_recv.at[i], partner).start()

    pl.loop(ahead, tiles)(within)

    @pl.loop(0, tiles)
    def _(j):
        pltpu.make_async_copy(intra.at[j], intra_ref.at[j], y_done.at[j]).wait()
        pltpu.make_async_copy(weight.at[j], weight_ref.at[j], w_done.at[j]).wait()
        pltpu.make_async_copy(prior.at[j], prior_ref.at[j], s_done.at[j]).wait()

    @pl.loop(0, half)
    def _(i):
        remote(gone.at[i], entry.at[theirs + i], e_send.at[i], e_recv.at[i], partner).wait_recv()
        remote(gone.at[i], entry.at[theirs + i], e_send.at[i], e_recv.at[i], partner).wait_send()
        remote(own.at[i], across.at[i], x_send.at[i], x_recv.at[i], column).wait_send()
        remote(paired.at[i], paired.at[i], p_send.at[i], p_recv.at[i], partner).wait_send()

        @pl.when(z < ZS - 1)
        def _():
            remote(leaving.at[i], arrived.at[i], z_send.at[i], z_recv.at[i], up).wait_send()

    for c in to_quad:
        c.wait_send()
    enter_ref[...] = entry[...]


def entering_states(cum, row, reach, turned, pre, decay, c_proj, b_proj, inner):
    tiles = row.shape[0]
    half = tiles // 2
    rows = inner.shape[0]
    chunks, size, _ = turned.shape
    tile = (size, CHUNK)
    vmem = pl.BlockSpec(memory_space=pltpu.VMEM)
    hbm = pl.BlockSpec(memory_space=pltpu.HBM)
    sems = pltpu.SemaphoreType.DMA
    like = lambda a: pltpu.VMEM(a.shape, a.dtype)
    return pl.pallas_call(
        exchange_kernel,
        out_shape=(
            jax.ShapeDtypeStruct((tiles,) + tile, BF16),
            jax.ShapeDtypeStruct((tiles, rows, CHUNK), F32),
            jax.ShapeDtypeStruct((tiles, rows, 2 * CHUNK), BF16),
            jax.ShapeDtypeStruct((tiles, chunks - 1) + tile, F32),
        ),
        in_specs=[hbm] * 5 + [vmem] + [hbm] * 3,
        out_specs=(vmem, hbm, hbm, hbm),
        scratch_shapes=[like(a) for a in (cum, row, reach, turned, pre, c_proj, b_proj, inner)] + [
            sems((8,)), pltpu.VMEM((tiles,) + tile, BF16), pltpu.VMEM((tiles, chunks - 1) + tile, F32), sems((tiles,)),
            pltpu.VMEM((4,) + decay.shape, F32)]
        + [pltpu.VMEM((half,) + tile, BF16)] * 6
        + [
            pltpu.VMEM((tiles,) + tile, BF16),
            pltpu.VMEM((tiles, rows, CHUNK), F32), pltpu.VMEM((tiles, rows, 2 * CHUNK), BF16),
            pltpu.VMEM((rows, CHUNK), F32), pltpu.VMEM((CHUNK, CHUNK), F32), sems((tiles,)), sems((tiles,)),
        ]
        + [sems((3,))] * 2 + [sems((half,))] * 8,
        compiler_params=pltpu.CompilerParams(collective_id=1, has_side_effects=True, vmem_limit_bytes=67043328),
        name="entering_states",
    )(cum, row, reach, turned, pre, decay, c_proj, b_proj, inner)


def reduce_kernel(part_ref, out_ref, paired, held, landed, own, copies, a_send, a_recv, b_send, b_recv, c_send, c_recv):
    place = place_of()
    core, dp = place["core"], place["dp"]
    peers, parts = held.shape[0], copies.shape[0]
    here = place["seq"] // 2
    partner = device_at(place, core=1 - core)

    def in_column(o):
        b = lax.rem(here + o, peers)
        return b, (dp, b * 2 + core)

    def in_dp(o):
        return (lax.rem(dp + o, parts), place["seq"])

    meet([partner] + [in_column(o)[1] for o in range(1, peers)] + [in_dp(o) for o in range(1, parts)])
    first = remote(part_ref.at[1 - core], paired, a_send, a_recv, partner)
    first.start()
    first.wait()
    held[...] = (part_ref[core].astype(F32) + paired[...].astype(F32)).astype(BF16)
    sent = []
    for o in range(1, peers):
        b, device = in_column(o)
        c = remote(held.at[b], landed.at[o - 1], b_send.at[o - 1], b_recv.at[o - 1], device)
        c.start()
        sent.append(c)
    total = held[here].astype(F32)
    for o in range(1, peers):
        sent[o - 1].wait_recv()
        total = total + landed[o - 1].astype(F32)
    own[...] = total.astype(BF16)
    copies[dp] = own[...]
    given = []
    for o in range(1, parts):
        c = remote(own, copies.at[dp], c_send.at[o - 1], c_recv.at[o - 1], in_dp(o))
        c.start()
        given.append(c)
    for o in range(1, parts):
        source = lax.rem(dp + parts - o, parts)
        remote(own, copies.at[source], c_send.at[o - 1], c_recv.at[o - 1], in_dp(o)).wait_recv()
    total = copies[0].astype(F32)
    for i in range(1, parts):
        total = total + copies[i].astype(F32)
    out_ref[...] = total
    for c in sent + given:
        c.wait_send()


def reduced_gradient(grad):
    block = grad.shape[2:]
    peers, parts = grad.shape[1], 8
    vmem = pl.BlockSpec(memory_space=pltpu.VMEM)
    sems = pltpu.SemaphoreType.DMA
    return pl.pallas_call(
        reduce_kernel,
        out_shape=jax.ShapeDtypeStruct(block, F32),
        in_specs=[vmem],
        out_specs=vmem,
        scratch_shapes=[
            pltpu.VMEM((peers,) + block, BF16), pltpu.VMEM((peers,) + block, BF16),
            pltpu.VMEM((peers - 1,) + block, BF16), pltpu.VMEM(block, BF16), pltpu.VMEM((parts,) + block, BF16),
            sems, sems, sems((peers - 1,)), sems((peers - 1,)), sems((parts - 1,)), sems((parts - 1,)),
        ],
        compiler_params=pltpu.CompilerParams(collective_id=2, has_side_effects=True),
        name="reduced_gradient",
    )(grad)


def body(tokens, w_x, w_bc, w_dt, dt_bias, decay_rate, gain, cotangent, counts):
    seq_tokens = tokens[0]
    cot_rows = cotangent[0]
    inner, b_proj, c_proj, dt_raw = gather_project(w_x, w_bc, w_dt, seq_tokens)
    cum, row, reach, turned, pre, decay = local_decays(
        dt_raw, dt_bias, decay_rate, counts, b_proj, inner.shape[1] // CHUNK)
    entering, intra, weight, prior = entering_states(cum, row, reach, turned, pre, decay, c_proj, b_proj, inner)
    outputs, grad = local_outputs(
        cum, c_proj, b_proj, counts, seq_tokens, inner, cot_rows, gain, intra, weight, prior, pre, entering)
    gradient = reduced_gradient(grad)
    return (outputs[None], gradient)


def solution(mesh):
    return jax.shard_map(
        body,
        mesh=mesh,
        in_specs=(
            P("dp", "seq", None), P("seq", None), P("seq", None), P("seq", None),
            P(), P(), P(), P("dp", "seq", None), P(),
        ),
        out_specs=(P("dp", "seq", None), P("seq", None)),
        check_vma=False,
    )
```

```python
import functools

import jax
import jax.numpy as jnp
from jax import lax
from jax.experimental import pallas as pl
from jax.experimental.pallas import tpu as pltpu
from jax.sharding import Mesh
from jax.sharding import PartitionSpec as P

L = 256
CHUNK = 128
WIDE = 256
LOG2E = 1.4426950408889634
F32 = jnp.float32
BF16 = jnp.bfloat16


def dot(a, b):
    return jnp.dot(a, b, preferred_element_type=F32)


def dot_lanes(a, b):
    return lax.dot_general(a, b, (((1,), (1,)), ((), ())), preferred_element_type=F32)


def iota(shape, dim):
    return lax.broadcasted_iota(jnp.int32, shape, dim)


def split3(x):
    hi = x.astype(BF16).astype(F32)
    mid = (x - hi).astype(BF16).astype(F32)
    return hi, mid, x - hi - mid


def packed3(x):
    hi, mid, lo = split3(x)
    low_lanes = iota(x.shape, 1) < 64
    first = jnp.where(low_lanes, hi, pltpu.roll(mid, 64, 1))
    second = jnp.where(low_lanes, lo, 0.0)
    return jnp.concatenate([first.astype(BF16), second.astype(BF16)], axis=1)


def head_select(depth, first_head, lanes_per_head, lanes=WIDE):
    k = iota((depth, lanes), 0)
    l = iota((depth, lanes), 1)
    hit = ((k & 63) == first_head + l // lanes_per_head) & (k < 192)
    return jnp.where(hit, 1.0, 0.0).astype(BF16)


def slots_used(counts_ref):
    filled = counts_ref[lax.axis_index("seq")]
    return [jnp.where(filled > k, 1.0, 0.0).astype(F32) for k in range(2)]


def decay_kernel(dt_ref, bias_ref, rate_ref, counts_ref, b_ref,
                 cum_ref, row_ref, to_end, b_turned, pre_ref, decay_ref, padded):
    rows = dt_ref.shape[0]
    chunks = rows // CHUNK
    heads = bias_ref.shape[1]
    padded[...] = jnp.zeros_like(padded)
    padded[0:1, :heads] = bias_ref[...]
    padded[1:2, :heads] = rate_ref[...]
    used = slots_used(counts_ref)
    v = dt_ref[...] + padded[0:1, :]
    dt = jnp.maximum(v, 0.0) + jnp.log1p(jnp.exp(-jnp.abs(v)))
    slot = iota(dt.shape, 0) // L
    dt = dt * jnp.where(slot == 0, used[0], used[1])
    drop = dt * (padded[1:2, :] * (-LOG2E))
    tri = jnp.where(iota((CHUNK, CHUNK), 0) >= iota((CHUNK, CHUNK), 1), 1.0, 0.0).astype(BF16)
    lasts = []
    for c in range(chunks):
        at = slice(c * CHUNK, (c + 1) * CHUNK)
        hi, mid, lo = split3(drop[at])
        cum = dot(tri, hi.astype(BF16)) + dot(tri, mid.astype(BF16)) + dot(tri, lo.astype(BF16))
        own = cum - jnp.log2(dt[at])
        last = cum[CHUNK - 1:CHUNK]
        lasts.append(last)
        cum_ref[at, :] = packed3(cum)
        reach = jnp.exp2(last - own)
        reach_hi = reach.astype(BF16).astype(F32)
        reach_lo = pltpu.roll(reach - reach_hi, 64, 1)
        to_end[at, :] = jnp.where(iota(reach.shape, 1) < 64, reach_hi, reach_lo).astype(BF16)
        turned = own.T
        for g in range(row_ref.shape[0]):
            row_ref[g, :, at] = turned[2 * g:2 * g + 2]
        b_turned[c] = b_ref[at, :].astype(F32).T.astype(BF16)
    drops = [jnp.exp2(last) for last in lasts]
    befores = [jnp.ones_like(drops[0])]
    for d in drops[:-1]:
        befores.append(befores[-1] * d)
    by_head = jnp.concatenate(befores + drops, axis=0)
    low_half = iota((2 * chunks, CHUNK), 1) < 64
    for j in range(pre_ref.shape[0]):
        low = jnp.broadcast_to(by_head[:, 2 * j:2 * j + 1], low_half.shape)
        high = jnp.broadcast_to(by_head[:, 2 * j + 1:2 * j + 2], low_half.shape)
        spread = jnp.where(low_half, low, high)
        pre_ref[j] = spread
        decay_ref[j:j + 1, :] = spread[chunks - 1:chunks] * spread[2 * chunks - 1:2 * chunks]


def output_kernel(cum_ref, c_ref, b_ref, counts_ref, tokens_ref, inner_ref, cot_ref, gain_ref, intra_ref, weight_ref,
                  prior_ref, pre_ref, enter_ref, out_ref, grad_ref, sum_heads, combined, through, full_grad):
    step = pl.program_id(0)
    rows = c_ref.shape[0]
    chunks = rows // CHUNK

    @pl.when(step == 0)
    def _():
        same = iota(sum_heads.shape, 0) // 64 == iota(sum_heads.shape, 1) // 64
        sum_heads[...] = jnp.where(same, 1.0, 0.0).astype(BF16)
        combined[...] = jnp.zeros_like(combined)
        through[...] = jnp.zeros_like(through)

    used = slots_used(counts_ref)
    low_half = iota((CHUNK, CHUNK), 1) < 64
    growths = jnp.exp2(dot(cum_ref[...], head_select(2 * CHUNK, step * 4, 64)))
    entry = jnp.concatenate([enter_ref[p].astype(F32) for p in range(2)], axis=1)
    for c in range(chunks):
        at = slice(c * CHUNK, (c + 1) * CHUNK)
        entering = entry * jnp.concatenate([pre_ref[p, c:c + 1, :] for p in range(2)], axis=1)
        if c > 0:
            entering = entering + jnp.concatenate([prior_ref[p, c - 1] for p in range(2)], axis=1)
        state_low = entering.astype(BF16)
        from_state = dot(c_ref[at, :], state_low) * growths[at]
        gain_row = gain_ref[...] * used[c * CHUNK // L]
        scaled = []
        for p in range(2):
            lanes = slice(p * CHUNK, (p + 1) * CHUNK)
            x = inner_ref[at, lanes]
            zero = jnp.zeros_like(x)
            heads = jnp.concatenate([jnp.where(low_half, x, zero), jnp.where(low_half, zero, x)], axis=0)
            full = intra_ref[p, at, :] + from_state[:, lanes]
            gain = gain_row[:, lanes]
            grad_out = cot_ref[at, lanes].astype(F32) * gain
            parts = jnp.concatenate([(full * full).astype(BF16), (grad_out * full).astype(BF16)], axis=1)
            sums = dot(parts, sum_heads[...])
            inverse = lax.rsqrt(sums[:, :CHUNK] * (1.0 / 64) + 1.0)
            normed = full * inverse
            out_ref[at, lanes] = (normed * gain).astype(BF16)
            grad = inverse * (grad_out - normed * (sums[:, CHUNK:] * inverse * (1.0 / 64)))
            inter = dot_lanes(grad.astype(BF16), heads) * weight_ref[p, at, :].astype(F32)
            combined[at, :] += inter[:, :CHUNK] + inter[:, CHUNK:]
            scaled.append((grad * growths[at, lanes]).astype(BF16))
        through[at, :] += dot_lanes(jnp.concatenate(scaled, axis=1), state_low)

    @pl.when(step == pl.num_programs(0) - 1)
    def _():
        turned = []
        for c in range(chunks):
            at = slice(c * CHUNK, (c + 1) * CHUNK)
            grad_rows = dot(combined[at, :].astype(BF16), b_ref[at, :]) + through[at, :]
            turned.append(grad_rows.astype(BF16).astype(F32).T.astype(BF16))
        turned = jnp.concatenate(turned, axis=1)
        for k in range(full_grad.shape[0] // CHUNK):
            at = slice(k * CHUNK, (k + 1) * CHUNK)
            full_grad[at, :] = dot(turned, tokens_ref[:, at]).T.astype(BF16)
        block = grad_ref.shape[2]
        for k in range(full_grad.shape[0] // block):
            grad_ref[k % 2, k // 2] = full_grad[k * block:(k + 1) * block, :]


MESH = pl.DeviceIdType.MESH
ZS = 8
CLASSES = {"A": 0, "B": 1, "X": 2, "D": 3}


def place_of():
    dp, seq = lax.axis_index("dp"), lax.axis_index("seq")
    return dict(y=dp // 2, x_lo=lax.rem(dp, 2), z=seq // 4, x_hi=lax.rem(seq // 2, 2), core=lax.rem(seq, 2), seq=seq, dp=dp)


def device_at(place, **new):
    p = {**place, **new}
    return (p["y"] * 2 + p["x_lo"], p["z"] * 4 + p["x_hi"] * 2 + p["core"])


def neighbours(place):
    z, y = place["z"], place["y"]
    flip = 1 - place["x_lo"]
    return dict(
        zp=device_at(place, z=lax.rem(z + 1, ZS)), zm=device_at(place, z=lax.rem(z + ZS - 1, ZS)),
        yp=device_at(place, y=lax.rem(y + 1, 4)), ym=device_at(place, y=lax.rem(y + 3, 4)),
        xu=device_at(place, x_lo=flip, x_hi=1 - place["x_hi"]), xo=device_at(place, x_lo=flip),
        partner=device_at(place, core=1 - place["core"]),
    )


def meet(devices):
    barrier = pltpu.get_barrier_semaphore()
    for d in devices:
        pl.semaphore_signal(barrier, inc=1, device_id=d, device_id_type=MESH)
    pl.semaphore_wait(barrier, len(devices))


ORDER = (
    ("A", -1, "0"), ("A", 1, "0"), ("A", -1, "1"), ("A", 1, "1"), ("X", 0, "u"), ("B", -1, "0"), ("A", -2, "0"),
    ("A", 2, "0"), ("D", 0, "u"), ("B", 1, "0"), ("B", -1, "1"), ("X", 0, "o"), ("A", -2, "1"), ("A", 2, "1"),
    ("X", -1, "u"), ("B", -2, "0"), ("B", 1, "1"), ("D", 0, "o"), ("C", 0, "Q"), ("A", -3, "0"), ("A", 3, "0"),
    ("X", 1, "u"), ("B", -2, "1"), ("B", 2, "0"), ("X", -1, "o"), ("C", 0, "R"), ("A", -3, "1"), ("A", 3, "1"),
    ("X", -2, "u"), ("B", 2, "1"), ("D", -1, "u"), ("C", -1, "Q"), ("X", 2, "u"), ("A", 4, "0"), ("X", 1, "o"),
    ("B", -3, "0"), ("D", -1, "o"), ("C", 1, "Q"), ("A", 4, "1"), ("X", -3, "u"), ("X", -2, "o"), ("D", -2, "u"),
    ("C", -1, "R"), ("B", -3, "1"), ("B", 3, "0"), ("X", 2, "o"), ("X", 3, "u"), ("C", -2, "Q"), ("D", -2, "o"),
    ("C", 2, "Q"), ("B", 3, "1"), ("D", 1, "u"), ("X", -3, "o"), ("X", 4, "u"), ("B", 4, "0"), ("D", 1, "o"),
    ("C", -2, "R"), ("D", -3, "u"), ("X", 3, "o"), ("C", -3, "Q"), ("C", 1, "R"), ("B", 4, "1"), ("C", 3, "Q"),
    ("D", 2, "u"), ("D", 4, "u"), ("D", 3, "u"), ("X", 4, "o"), ("D", 2, "o"), ("C", 4, "Q"), ("D", -3, "o"),
    ("D", 3, "o"), ("D", 4, "o"), ("C", 2, "R"), ("C", -3, "R"), ("C", 3, "R"), ("C", 4, "R"),
)
FAR = ("x", "y", "z", "x", "y")


def gather_kernel(wx_ref, wbc_ref, wdt_ref, tokens_ref, inner_ref, b_ref, c_ref, dt_ref,
                  held, cut, total, own_sem, send_sem, in_sem, side_sem, shard_sem):
    place = place_of()
    near = neighbours(place)
    core, x_lo, x_hi, z, y = (place[k] for k in ("core", "x_lo", "x_hi", "z", "y"))
    me = place["seq"]
    quarter = held.shape[3]
    y_lo = lax.rem(y, 2)
    depth = cut.shape[2]
    width = wx_ref.shape[1]

    loads = [pltpu.make_async_copy(wx_ref.at[:, pl.ds(q * quarter, quarter)], held.at[q, me], own_sem.at[q]) for q in range(3)]
    tail = width - 3 * quarter
    loads.append(pltpu.make_async_copy(wx_ref.at[:, pl.ds(3 * quarter, tail)], held.at[3, me, :, pl.ds(0, tail)], own_sem.at[3]))
    loads.append(pltpu.make_async_copy(wbc_ref, held.at[3, me, :, pl.ds(tail, wbc_ref.shape[1])], own_sem.at[4]))
    for c in loads:
        c.start()
    spare = quarter - tail - wbc_ref.shape[1] - wdt_ref.shape[1]
    held[3, me, :, tail + wbc_ref.shape[1]:] = jnp.concatenate(
        [wdt_ref[...].astype(F32), jnp.zeros((wdt_ref.shape[0], spare), F32)], axis=1).astype(BF16)
    meet(list(near.values()))
    for c in loads:
        c.wait()

    sent = []

    def unit(cls, dz, r):
        q = core * 2 + (y_lo if cls in "AX" else 1 - y_lo)
        xh = x_hi if cls in "AB" else 1 - x_hi
        return held.at[q, lax.rem(z + dz + ZS, ZS) * 4 + xh * 2 + r]

    def index(cls, dz, r):
        return CLASSES[cls] * 16 + (dz % ZS) * 2 + r

    def send(cls, dz, r, device, as_cls, as_dz, sem):
        ref = unit(cls, dz, r)
        c = pltpu.make_async_remote_copy(
            src_ref=ref, dst_ref=ref, send_sem=send_sem.at[len(sent)], recv_sem=sem.at[index(as_cls, as_dz, r)],
            device_id=device, device_id_type=MESH)
        c.start()
        sent.append(c)

    def arrive(cls, dz, r):
        ref = unit(cls, dz, r)
        pltpu.make_async_remote_copy(
            src_ref=ref, dst_ref=ref, send_sem=send_sem.at[0], recv_sem=in_sem.at[index(cls, dz, r)],
            device_id=near["partner"], device_id_type=MESH).wait_recv()

    def aside(cls, dz, r):
        send(cls, dz, r, near["partner"], cls, dz, side_sem)

    def along_y(r):
        return device_at(place, y=lax.rem(y + 5 - 2 * r, 4))

    shard = held.at[:, me]
    shard_copy = pltpu.make_async_remote_copy(
        src_ref=shard, dst_ref=shard, send_sem=shard_sem.at[0], recv_sem=shard_sem.at[1],
        device_id=near["partner"], device_id_type=MESH)
    shard_copy.start()
    r_u, r_o = x_lo, 1 - x_lo
    send("A", 0, core, near["zp"], "A", -1, in_sem)
    send("A", 0, core, near["zm"], "A", 1, in_sem)

    for i in range(ZS):
        cut[i] = tokens_ref[:, i * depth:(i + 1) * depth]
    total[...] = jnp.zeros_like(total)

    other = held.at[:, me + 1 - 2 * core]
    pltpu.make_async_remote_copy(
        src_ref=other, dst_ref=other, send_sem=shard_sem.at[0], recv_sem=shard_sem.at[1],
        device_id=near["partner"], device_id_type=MESH).wait_recv()
    send("A", 0, 1 - core, near["zp"], "A", -1, in_sem)
    send("A", 0, 1 - core, near["zm"], "A", 1, in_sem)
    send("A", 0, r_o, near["xu"], "X", 0, in_sem)
    send("B", 0, r_o, near["xu"], "D", 0, in_sem)
    first = set()
    for kind, dz, which in ORDER:
        if kind != "C":
            r = {"0": 0, "1": 1, "u": r_u, "o": r_o}[which]
            arrive(kind, dz, r)
        pair_done = (kind, dz) in first
        first.add((kind, dz))
        if kind == "A":
            if dz < 0 and (dz > -3 or r == 0):
                send("A", dz, r, near["zp"], "A", dz - 1, in_sem)
            if 0 < dz < 4 and (dz < 3 or r == 1):
                send("A", dz, r, near["zm"], "A", dz + 1, in_sem)
            send("A", dz, r, near["yp" if r == 0 else "ym"], "B", dz, in_sem)
            if pair_done:
                send("A", dz, r_o, near["xu"], "X", dz, in_sem)
            aside("A", dz, r)
        elif kind == "B":
            if pair_done and FAR[abs(dz)] == "x":
                send("B", dz, r_o, near["xu"], "D", dz, in_sem)
            aside("B", dz, r)
        elif kind == "X":
            if which == "u":
                send("X", dz, r, near["xo"], "X", dz, in_sem)
            if FAR[abs(dz)] == "y":
                send("X", dz, r, along_y(r), "D", dz, in_sem)
            aside("X", dz, r)
        elif kind == "D":
            if which == "u" and FAR[abs(dz)] == "x":
                send("D", dz, r, near["xo"], "D", dz, in_sem)
            if -3 < dz <= 0 and FAR[abs(dz) + 1] == "z":
                send("D", dz, r, near["zp"], "D", dz - 1, in_sem)
            if 0 <= dz < 3 and FAR[abs(dz) + 1] == "z":
                send("D", dz, r, near["zm"], "D", dz + 1, in_sem)
            aside("D", dz, r)
        else:
            own = which == "Q"
            for cls in (("A" if own else "B") if dz else "") + ("X" if own else "D"):
                for r in (0, 1):
                    q = (1 - core) * 2 + (y_lo if cls in "AX" else 1 - y_lo)
                    xh = x_hi if cls in "AB" else 1 - x_hi
                    ref = held.at[q, lax.rem(z + dz + ZS, ZS) * 4 + xh * 2 + r]
                    pltpu.make_async_remote_copy(
                        src_ref=ref, dst_ref=ref, send_sem=send_sem.at[0], recv_sem=side_sem.at[index(cls, dz, r)],
                        device_id=near["partner"], device_id_type=MESH).wait_recv()
            zq = lax.rem(z + dz + ZS, ZS)

            quarters = y_lo if own else 1 - y_lo

            @pl.loop(0, 2)
            def _(i, quarters=quarters, zq=zq):
                q = 2 * i + quarters
                block = held[q, pl.ds(zq * 4, 4)].reshape(depth, quarter)
                total[q] += dot(cut[zq], block)

    for q in range(3):
        inner_ref[:, q * quarter:(q + 1) * quarter] = total[q].astype(BF16)
    inner_ref[:, 3 * quarter:] = total[3, :, :tail].astype(BF16)
    b_ref[...] = total[3, :, tail:tail + 128].astype(BF16)
    c_ref[...] = total[3, :, tail + 128:tail + 256].astype(BF16)
    dt_ref[...] = total[3, :, tail + 256:tail + 384]
    shard_copy.wait_send()
    for c in sent:
        c.wait_send()


def gather_project(w_x, w_bc, w_dt, tokens):
    rows, depth = tokens.shape
    width = w_x.shape[1]
    quarter = (width + 512) // 4
    vmem = pl.BlockSpec(memory_space=pltpu.VMEM)
    hbm = pl.BlockSpec(memory_space=pltpu.HBM)
    return pl.pallas_call(
        gather_kernel,
        out_shape=(
            jax.ShapeDtypeStruct((rows, width), BF16),
            jax.ShapeDtypeStruct((rows, 128), BF16),
            jax.ShapeDtypeStruct((rows, 128), BF16),
            jax.ShapeDtypeStruct((rows, 128), F32),
        ),
        in_specs=[hbm, hbm, vmem, vmem],
        out_specs=(vmem,) * 4,
        scratch_shapes=[
            pltpu.VMEM((4, 32, w_x.shape[0], quarter), BF16),
            pltpu.VMEM((ZS, rows, depth // ZS), BF16),
            pltpu.VMEM((4, rows, quarter), F32),
            pltpu.SemaphoreType.DMA((5,)),
            pltpu.SemaphoreType.DMA((160,)),
            pltpu.SemaphoreType.DMA((64,)),
            pltpu.SemaphoreType.DMA((64,)),
            pltpu.SemaphoreType.DMA((2,)),
        ],
        compiler_params=pltpu.CompilerParams(collective_id=0, has_side_effects=True, vmem_limit_bytes=67043328),
        name="gather_project",
    )(w_x, w_bc, w_dt, tokens)


def whole(shape):
    return pl.BlockSpec(shape, lambda j: (0,) * len(shape))


def local_decays(dt_raw, dt_bias, decay_rate, counts, b_proj, tiles):
    rows, state_size = b_proj.shape
    chunks = rows // CHUNK
    vmem = pl.BlockSpec(memory_space=pltpu.VMEM)
    return pl.pallas_call(
        decay_kernel,
        out_shape=(
            jax.ShapeDtypeStruct((rows, 2 * CHUNK), BF16),
            jax.ShapeDtypeStruct((tiles, 2, rows), F32),
            jax.ShapeDtypeStruct((rows, CHUNK), BF16),
            jax.ShapeDtypeStruct((chunks, state_size, CHUNK), BF16),
            jax.ShapeDtypeStruct((tiles, 2 * chunks, CHUNK), F32),
            jax.ShapeDtypeStruct((tiles, CHUNK), F32),
        ),
        in_specs=[vmem, vmem, vmem, pl.BlockSpec(memory_space=pltpu.SMEM), vmem],
        out_specs=(vmem,) * 6,
        scratch_shapes=[pltpu.VMEM((8, 128), F32)],
        name="decays",
    )(dt_raw, dt_bias[None], decay_rate[None], counts, b_proj)


def local_outputs(cum, c_proj, b_proj, counts, tokens, inner, cot, gain, intra, weight, prior, pre, entering):
    rows, width = inner.shape
    depth = tokens.shape[1]
    state_size = b_proj.shape[1]
    steps = width // WIDE
    chunks = rows // CHUNK
    owners = 32
    tiles = WIDE // CHUNK
    columns = lambda r: pl.BlockSpec((r, WIDE), lambda j: (0, j))
    tiled = lambda a, b: pl.BlockSpec((tiles, a, b), lambda j: (j, 0, 0))
    grad_shape = (2, owners // 2, depth // owners, state_size)
    return pl.pallas_call(
        output_kernel,
        grid=(steps,),
        out_shape=(
            jax.ShapeDtypeStruct((rows, width), BF16),
            jax.ShapeDtypeStruct(grad_shape, BF16),
        ),
        in_specs=[
            whole((rows, 2 * CHUNK)), whole((rows, state_size)), whole((rows, state_size)),
            pl.BlockSpec(memory_space=pltpu.SMEM), whole((rows, depth)),
            columns(rows), columns(rows), columns(1), tiled(rows, CHUNK), tiled(rows, WIDE),
            pl.BlockSpec((tiles, chunks - 1, state_size, CHUNK), lambda j: (j, 0, 0, 0)),
            tiled(2 * chunks, CHUNK), tiled(state_size, CHUNK),
        ],
        out_specs=(columns(rows), whole(grad_shape)),
        scratch_shapes=[
            pltpu.VMEM((WIDE, WIDE), BF16),
            pltpu.VMEM((rows, CHUNK), F32),
            pltpu.VMEM((rows, CHUNK), F32),
            pltpu.VMEM((depth, state_size), BF16),
        ],
        name="outputs",
    )(cum, c_proj, b_proj, counts, tokens, inner, cot, gain[None], intra, weight, prior, pre, entering)


def remote(src, dst, send_sem, recv_sem, device):
    return pltpu.make_async_remote_copy(
        src_ref=src, dst_ref=dst, send_sem=send_sem, recv_sem=recv_sem, device_id=device, device_id_type=MESH)


LAG = (6, 4)


def exchange_kernel(cum_in, row_in, reach_in, turned_in, pre_in, decay_ref, c_in, b_in, inner_in,
                    enter_ref, intra_ref, weight_ref, prior_ref,
                    cum_ref, row_ref, reach_ref, turned_ref, pre_ref, c_ref, b_ref, inner_ref, load_sem,
                    state, prior, s_done,
                    decays, paired, across, own, arrived, leaving, gone, entry, intra, weight, gram, hide, y_done, w_done,
                    d_send, d_recv, p_send, p_recv, x_send, x_recv, z_send, z_recv, e_send, e_recv):
    loads = [pltpu.make_async_copy(a, b, load_sem.at[i]) for i, (a, b) in enumerate((
        (inner_in, inner_ref), (reach_in, reach_ref), (turned_in, turned_ref), (pre_in, pre_ref),
        (cum_in, cum_ref), (row_in, row_ref), (c_in, c_ref), (b_in, b_ref)))]
    for c in loads:
        c.start()
    place = place_of()
    core, x_hi, z = place["core"], place["x_hi"], place["z"]
    partner = device_at(place, core=1 - core)
    column = device_at(place, x_hi=1 - x_hi)
    corner = device_at(place, x_hi=1 - x_hi, core=1 - core)
    up = device_at(place, z=lax.rem(z + 1, ZS))
    down = device_at(place, z=lax.rem(z + ZS - 1, ZS))
    half = state.shape[0] // 2
    chunks = prior.shape[1] + 1
    mine, theirs = core * half, (1 - core) * half
    member = x_hi * 2 + core

    meet([partner, column, corner, up, down])
    to_quad = [remote(decay_ref, decays.at[member], d_send.at[i], d_recv.at[i], d)
               for i, d in enumerate((partner, column, corner))]
    to_quad[0].start()
    to_quad[1].start()
    to_quad[2].start()
    for c in loads:
        c.wait()

    def pair_of(j):
        return inner_ref[:, pl.ds(pl.multiple_of(j * CHUNK, CHUNK), CHUNK)]

    def added(j):
        reach = dot(reach_ref[...], head_select(CHUNK, 2 * j, 64, CHUNK))
        scaled = (pair_of(j).astype(F32) * reach).astype(BF16)
        now = dot(turned_ref[0], scaled[:CHUNK])
        for c in range(1, chunks):
            prior[j, c - 1] = now
            now = now * pre_ref[j, chunks + c:chunks + c + 1, :] + dot(turned_ref[c], scaled[c * CHUNK:(c + 1) * CHUNK])
        pltpu.make_async_copy(prior.at[j], prior_ref.at[j], s_done.at[j]).start()
        state[j] = now.astype(BF16)

    decays[member] = decay_ref[...]

    @pl.when(z == 0)
    def _():
        arrived[...] = jnp.zeros_like(arrived)

    for c, i in zip(to_quad, range(3)):
        remote(decay_ref, decays.at[(member ^ (1, 2, 3)[i])], d_send.at[i], d_recv.at[i], partner).wait_recv()

    def both_cores(i):
        remote(paired.at[i], paired.at[i], p_send.at[i], p_recv.at[i], partner).wait_recv()

    def leave(i):
        added(theirs + i)
        remote(state.at[theirs + i], paired.at[i], p_send.at[i], p_recv.at[i], partner).start()
        added(mine + i)

    def join(i):
        at = mine + i
        both_cores(i)
        own_state, other_state = state[at].astype(F32), paired[i].astype(F32)
        first = jnp.where(core == 0, own_state, other_state)
        second = jnp.where(core == 0, other_state, own_state)
        own[i] = (first * decays[x_hi * 2 + 1, pl.ds(at, 1), :] + second).astype(BF16)
        remote(own.at[i], across.at[i], x_send.at[i], x_recv.at[i], column).start()

    for c in range(chunks):
        at = slice(c * CHUNK, (c + 1) * CHUNK)
        gram[at, :] = dot_lanes(c_ref[at, :], b_ref[at, :])
    hide[...] = jnp.where(iota(hide.shape, 0) >= iota(hide.shape, 1), 0.0, -1e30)
    tiles = intra.shape[0]

    def within(j):
        spread = dot(cum_ref[...], head_select(2 * CHUNK, 2 * j, CHUNK))
        low_half = iota((CHUNK, CHUNK), 1) < 64
        pair = pair_of(j)
        for c in range(chunks):
            at = slice(c * CHUNK, (c + 1) * CHUNK)
            w0 = jnp.exp2(spread[at, :CHUNK] - row_ref[j, 0:1, at] + hide[...])
            w1 = jnp.exp2(spread[at, CHUNK:] - row_ref[j, 1:2, at] + hide[...])
            dots = gram[at, :]
            mixing = jnp.concatenate([(dots * w0).astype(BF16), (dots * w1).astype(BF16)], axis=1)
            weight[j, at, :] = jnp.concatenate([w0.astype(BF16), w1.astype(BF16)], axis=1)
            x = pair[at]
            zero = jnp.zeros_like(x)
            heads = jnp.concatenate([jnp.where(low_half, x, zero), jnp.where(low_half, zero, x)], axis=0)
            intra[j, at, :] = dot(mixing, heads)
        pltpu.make_async_copy(intra.at[j], intra_ref.at[j], y_done.at[j]).start()
        pltpu.make_async_copy(weight.at[j], weight_ref.at[j], w_done.at[j]).start()

    def chain(i):
        at = mine + i
        d = [decays[m, pl.ds(at, 1), :] for m in range(4)]
        remote(own.at[i], across.at[i], x_send.at[i], x_recv.at[i], column).wait_recv()
        mine_t, other_t = own[i].astype(F32), across[i].astype(F32)
        t0 = jnp.where(x_hi == 0, mine_t, other_t)
        t1 = jnp.where(x_hi == 0, other_t, mine_t)
        d0, d1 = d[0] * d[1], d[2] * d[3]

        @pl.when(z > 0)
        def _():
            remote(arrived.at[i], arrived.at[i], z_send.at[i], z_recv.at[i], down).wait_recv()

        before = arrived[i].astype(F32)

        @pl.when(z < ZS - 1)
        def _():
            leaving[i] = (before * (d0 * d1) + (t0 * d1 + t1)).astype(BF16)
            remote(leaving.at[i], arrived.at[i], z_send.at[i], z_recv.at[i], up).start()

        here = jnp.where(x_hi == 0, before, before * d0 + t0)
        first = jnp.where(core == 0, state[at].astype(F32), paired[i].astype(F32))
        after = here * jnp.where(x_hi == 0, d[0], d[2]) + first
        entry[at] = jnp.where(core == 0, here, after).astype(BF16)
        gone[i] = jnp.where(core == 0, after, here).astype(BF16)
        remote(gone.at[i], entry.at[at], e_send.at[i], e_recv.at[i], partner).start()

    lag = LAG[0] + LAG[1] * z
    slots = half + tiles
    length = jnp.maximum(slots, lag + half)

    @pl.loop(0, length)
    def _(slot):
        @pl.when(slot < half)
        def _():
            leave(slot)

        @pl.when((slot >= 2) & (slot < half + 2))
        def _():
            join(slot - 2)

        @pl.when((slot >= half) & (slot < slots))
        def _():
            within(slot - half)

        @pl.when((slot >= lag) & (slot < lag + half))
        def _():
            chain(slot - lag)

    @pl.loop(0, tiles)
    def _(j):
        pltpu.make_async_copy(intra.at[j], intra_ref.at[j], y_done.at[j]).wait()
        pltpu.make_async_copy(weight.at[j], weight_ref.at[j], w_done.at[j]).wait()
        pltpu.make_async_copy(prior.at[j], prior_ref.at[j], s_done.at[j]).wait()

    @pl.loop(0, half)
    def _(i):
        remote(gone.at[i], entry.at[theirs + i], e_send.at[i], e_recv.at[i], partner).wait_recv()
        remote(gone.at[i], entry.at[theirs + i], e_send.at[i], e_recv.at[i], partner).wait_send()
        remote(own.at[i], across.at[i], x_send.at[i], x_recv.at[i], column).wait_send()
        remote(paired.at[i], paired.at[i], p_send.at[i], p_recv.at[i], partner).wait_send()

        @pl.when(z < ZS - 1)
        def _():
            remote(leaving.at[i], arrived.at[i], z_send.at[i], z_recv.at[i], up).wait_send()

    for c in to_quad:
        c.wait_send()
    enter_ref[...] = entry[...]


def entering_states(cum, row, reach, turned, pre, decay, c_proj, b_proj, inner):
    tiles = row.shape[0]
    half = tiles // 2
    rows = inner.shape[0]
    chunks, size, _ = turned.shape
    tile = (size, CHUNK)
    vmem = pl.BlockSpec(memory_space=pltpu.VMEM)
    hbm = pl.BlockSpec(memory_space=pltpu.HBM)
    sems = pltpu.SemaphoreType.DMA
    like = lambda a: pltpu.VMEM(a.shape, a.dtype)
    return pl.pallas_call(
        exchange_kernel,
        out_shape=(
            jax.ShapeDtypeStruct((tiles,) + tile, BF16),
            jax.ShapeDtypeStruct((tiles, rows, CHUNK), F32),
            jax.ShapeDtypeStruct((tiles, rows, 2 * CHUNK), BF16),
            jax.ShapeDtypeStruct((tiles, chunks - 1) + tile, F32),
        ),
        in_specs=[hbm] * 5 + [vmem] + [hbm] * 3,
        out_specs=(vmem, hbm, hbm, hbm),
        scratch_shapes=[like(a) for a in (cum, row, reach, turned, pre, c_proj, b_proj, inner)] + [
            sems((8,)), pltpu.VMEM((tiles,) + tile, BF16), pltpu.VMEM((tiles, chunks - 1) + tile, F32), sems((tiles,)),
            pltpu.VMEM((4,) + decay.shape, F32)]
        + [pltpu.VMEM((half,) + tile, BF16)] * 6
        + [
            pltpu.VMEM((tiles,) + tile, BF16),
            pltpu.VMEM((tiles, rows, CHUNK), F32), pltpu.VMEM((tiles, rows, 2 * CHUNK), BF16),
            pltpu.VMEM((rows, CHUNK), F32), pltpu.VMEM((CHUNK, CHUNK), F32), sems((tiles,)), sems((tiles,)),
        ]
        + [sems((3,))] * 2 + [sems((half,))] * 8,
        compiler_params=pltpu.CompilerParams(collective_id=1, has_side_effects=True, vmem_limit_bytes=67043328),
        name="entering_states",
    )(cum, row, reach, turned, pre, decay, c_proj, b_proj, inner)


def reduce_kernel(part_ref, out_ref, paired, held, landed, own, copies, a_send, a_recv, b_send, b_recv, c_send, c_recv):
    place = place_of()
    core, dp = place["core"], place["dp"]
    peers, parts = held.shape[0], copies.shape[0]
    here = place["seq"] // 2
    partner = device_at(place, core=1 - core)

    def in_column(o):
        b = lax.rem(here + o, peers)
        return b, (dp, b * 2 + core)

    def in_dp(o):
        return (lax.rem(dp + o, parts), place["seq"])

    meet([partner] + [in_column(o)[1] for o in range(1, peers)] + [in_dp(o) for o in range(1, parts)])
    first = remote(part_ref.at[1 - core], paired, a_send, a_recv, partner)
    first.start()
    first.wait()
    held[...] = (part_ref[core].astype(F32) + paired[...].astype(F32)).astype(BF16)
    sent = []
    for o in range(1, peers):
        b, device = in_column(o)
        c = remote(held.at[b], landed.at[o - 1], b_send.at[o - 1], b_recv.at[o - 1], device)
        c.start()
        sent.append(c)
    total = held[here].astype(F32)
    for o in range(1, peers):
        sent[o - 1].wait_recv()
        total = total + landed[o - 1].astype(F32)
    own[...] = total.astype(BF16)
    copies[dp] = own[...]
    given = []
    for o in range(1, parts):
        c = remote(own, copies.at[dp], c_send.at[o - 1], c_recv.at[o - 1], in_dp(o))
        c.start()
        given.append(c)
    for o in range(1, parts):
        source = lax.rem(dp + parts - o, parts)
        remote(own, copies.at[source], c_send.at[o - 1], c_recv.at[o - 1], in_dp(o)).wait_recv()
    total = copies[0].astype(F32)
    for i in range(1, parts):
        total = total + copies[i].astype(F32)
    out_ref[...] = total
    for c in sent + given:
        c.wait_send()


def reduced_gradient(grad):
    block = grad.shape[2:]
    peers, parts = grad.shape[1], 8
    vmem = pl.BlockSpec(memory_space=pltpu.VMEM)
    sems = pltpu.SemaphoreType.DMA
    return pl.pallas_call(
        reduce_kernel,
        out_shape=jax.ShapeDtypeStruct(block, F32),
        in_specs=[vmem],
        out_specs=vmem,
        scratch_shapes=[
            pltpu.VMEM((peers,) + block, BF16), pltpu.VMEM((peers,) + block, BF16),
            pltpu.VMEM((peers - 1,) + block, BF16), pltpu.VMEM(block, BF16), pltpu.VMEM((parts,) + block, BF16),
            sems, sems, sems((peers - 1,)), sems((peers - 1,)), sems((parts - 1,)), sems((parts - 1,)),
        ],
        compiler_params=pltpu.CompilerParams(collective_id=2, has_side_effects=True),
        name="reduced_gradient",
    )(grad)


def body(tokens, w_x, w_bc, w_dt, dt_bias, decay_rate, gain, cotangent, counts):
    seq_tokens = tokens[0]
    cot_rows = cotangent[0]
    inner, b_proj, c_proj, dt_raw = gather_project(w_x, w_bc, w_dt, seq_tokens)
    cum, row, reach, turned, pre, decay = local_decays(
        dt_raw, dt_bias, decay_rate, counts, b_proj, inner.shape[1] // CHUNK)
    entering, intra, weight, prior = entering_states(cum, row, reach, turned, pre, decay, c_proj, b_proj, inner)
    outputs, grad = local_outputs(
        cum, c_proj, b_proj, counts, seq_tokens, inner, cot_rows, gain, intra, weight, prior, pre, entering)
    gradient = reduced_gradient(grad)
    return (outputs[None], gradient)


def solution(mesh):
    return jax.shard_map(
        body,
        mesh=mesh,
        in_specs=(
            P("dp", "seq", None), P("seq", None), P("seq", None), P("seq", None),
            P(), P(), P(), P("dp", "seq", None), P(),
        ),
        out_specs=(P("dp", "seq", None), P("seq", None)),
        check_vma=False,
    )
```
